256 devices in a mesh: grp: 2 (over y), row: 128 (over z, x, core).
Axes of the slice: x: 4, y: 2, z: 16, core: 2. Of those that a mesh axis runs over, the one named last changes fastest.
The devices are a block of a 4x16x16 slice.
Arguments:
- cells: float32 [2048, 128, 192], P(('grp', 'row')), parts along dimension 0, may hold values from -6 to 6
- n_train: int32 [2], P('grp'), parts along dimension 0, may hold values from 128 to 1023
- present: int32 [256], P('grp'), parts along dimension 0, may hold values from 0 to 1, as said below
- norm_gain: float32 [3, 192], replicated, may hold values from 0.1 to 1.9
- feat_qkv: bfloat16 [3, 192, 192], replicated, may hold values from -6 to 6
- feat_out: bfloat16 [192, 192], replicated, may hold values from -0.4375 to 0.4375
- item_qkv: bfloat16 [3, 192, 192], replicated, may hold values from -6 to 6
- item_out: bfloat16 [192, 192], replicated, may hold values from -0.875 to 0.875
- mlp_in: bfloat16 [192, 768], replicated, may hold values from -0.4375 to 0.4375
- mlp_out: bfloat16 [768, 192], replicated, may hold values from -0.21875 to 0.21875
Outputs:
- result: float32 [2048, 128, 192], P(('grp', 'row')), parts along dimension 0
The draws below stay inside these ranges and needn't reach their ends.
There are 2 independent parts, one for each index of `grp`. The reference program is written for one: setup_inputs(seed, part) draws one part's arguments, and reference() takes and returns one part's arrays. A program takes and returns all parts, laid end to end along the dimension named above; an argument that names none is the same for every part. Nothing has to cross between parts.
Inputs may be any that keep to these rules, and one draw needn't show every extreme that they name: At least one of the 128 features is present.
All inputs are finite; a program needn't handle non-finite values.
Results may differ from the reference program's by a relative error of at most 0.03.
The reference program's roundings to bfloat16 on the way count: a program that leaves them out, or rounds other values in their place, can miss the bound.
Values may be sent and summed in bfloat16 or wider, within the bound.
No kernel may reach another device: no remote copies, remote signals or barrier semaphores. Data moves between devices by JAX's collectives and lax.ppermute only.
A program may use at most 64 MiB of HBM per device.

```python
import math
import jax
import jax.numpy as jnp
from jax import lax

E = 192
HEADS = 6
FF = 768
FEAT = 128
ROWS = 1024


def drawn_triplet(key):
    base = jax.random.normal(key, (3, E, E), jnp.float32) / math.sqrt(E)
    stacked = jnp.stack([3.0 * base[0], 3.0 * base[1], base[2]])
    return jnp.clip(stacked, -6.0, 6.0).astype(jnp.bfloat16)


def draw_feat_qkv(key, part):
    return drawn_triplet(jax.random.fold_in(key, 11))


def draw_item_qkv(key, part):
    return drawn_triplet(jax.random.fold_in(key, 23))


def draw_present(key, part):
    levels = jax.random.randint(jax.random.fold_in(key, 5), (FEAT,), 0, 4)
    forced = jax.random.randint(jax.random.fold_in(key, 6), (), 0, FEAT)
    position = jnp.arange(FEAT, dtype=jnp.int32)
    return jnp.where((levels > 0) | (position == forced), 1, 0).astype(jnp.int32)


def block_levels(rng, dims, cuts, smallest, high):
    def one(dim, blocks):
        draws = jax.random.uniform(jax.random.fold_in(jax.random.fold_in(rng, 6), dim), (blocks,), jnp.float32, smallest / len(cuts), high / len(cuts))
        return jnp.repeat(jnp.exp(draws), dims[dim] // blocks).reshape((-1,) + (1,) * (len(dims) - dim - 1))

    loudness = one(*cuts[0])
    for cut in cuts[1:]:
        loudness = loudness * one(*cut)
    return loudness


def bell_draw(key, dims, width, bound, pieces=(), kind=jnp.bfloat16):
    values = jax.random.normal(key, dims, jnp.float32) * width
    if len(pieces) > 0:
        values = block_levels(key, dims, pieces, -0.22, 0.18) * values
    return jnp.clip(values, min=-bound, max=bound).astype(kind)


def setup_inputs(seed: int = 0, part: int = 0) -> dict:
    splits = jax.random.split(jax.random.key(seed), 11)
    own_keys = jax.random.split(jax.random.fold_in(splits[10], part), 11)
    return {
        "cells": bell_draw(own_keys[0], (ROWS, FEAT, E), 1.0, 6.0, ((0, 128),), jnp.float32),
        "n_train": jax.random.randint(own_keys[1], (1,), ROWS // 8, ROWS).astype(jnp.int32),
        "present": draw_present(jax.random.fold_in(jax.random.fold_in(splits[10], part), 71), part),
        "norm_gain": jnp.clip(1.0 + 0.18 * jax.random.normal(splits[3], (3, E), jnp.float32), 0.1, 1.9),
        "feat_qkv": draw_feat_qkv(jax.random.fold_in(splits[10], 71), part),
        "feat_out": bell_draw(splits[5], (E, E), E ** -0.5, 0.4375),
        "item_qkv": draw_item_qkv(jax.random.fold_in(splits[10], 71), part),
        "item_out": bell_draw(splits[7], (E, E), (E // 4) ** -0.5, 0.875),
        "mlp_in": bell_draw(splits[8], (E, FF), E ** -0.5, 0.4375),
        "mlp_out": bell_draw(splits[9], (FF, E), FF ** -0.5, 0.21875),
    }


norm_floor = 0.25
masked_score = -1e+30

def widen(array):
    return array.astype(jnp.float32)

def layer_norm(stream, gain):
    average = lax.optimization_barrier(jnp.mean(stream, axis=-1, keepdims=True))
    centred = stream - average
    spread = lax.optimization_barrier(jnp.mean(centred * centred, axis=-1, keepdims=True))
    return centred * lax.rsqrt(spread + norm_floor) * gain

def softmax_rows(scores):
    largest = lax.optimization_barrier(jnp.max(scores, axis=-1, keepdims=True))
    exponent = jnp.exp(scores - largest)
    return exponent / lax.optimization_barrier(jnp.sum(exponent, axis=-1, keepdims=True))

def reference(cells, n_train, present, norm_gain, feat_qkv, feat_out, item_qkv, item_out, mlp_in, mlp_out):
    head_size = E // HEADS
    scale = 1.0 / math.sqrt(head_size)
    row_group = math.gcd(ROWS, 128)
    query_rows = min(512, ROWS)
    highest = lax.Precision.HIGHEST

    def feature_group(stream):
        normed = layer_norm(stream, norm_gain[0]).astype(jnp.bfloat16)
        triplet = jnp.einsum('rfe,ced->crfd', widen(normed), widen(feat_qkv))
        triplet = triplet.reshape(3, row_group, FEAT, HEADS, head_size)
        values = widen(triplet[2].astype(jnp.bfloat16))
        scores = jnp.einsum('rfhd,rghd->rhfg', triplet[0], triplet[1], precision=highest) * scale
        scores = jnp.where(present[None, None, None, :] > 0, scores, masked_score)
        weights = softmax_rows(scores).astype(jnp.bfloat16)
        context = jnp.einsum('rhfg,rghd->rfhd', widen(weights), values).astype(jnp.bfloat16)
        context = context.reshape(row_group, FEAT, E)
        return stream + jnp.dot(context, feat_out, preferred_element_type=jnp.float32)
    cells_mid = lax.map(feature_group, cells.reshape(ROWS // row_group, row_group, FEAT, E)).reshape(ROWS, FEAT, E)
    key_live = jnp.arange(ROWS, dtype=jnp.int32) < n_train[0]

    def item_feature(stream):
        normed = layer_norm(stream, norm_gain[1]).astype(jnp.bfloat16)
        triplet = jnp.einsum('re,ced->crd', widen(normed), widen(item_qkv))
        keys = triplet[1].reshape(ROWS, HEADS, head_size)
        values = widen(triplet[2].astype(jnp.bfloat16)).reshape(ROWS, HEADS, head_size)
        queries = triplet[0].reshape(ROWS // query_rows, query_rows, HEADS, head_size)

        def query_group(chosen):
            scores = jnp.einsum('qhd,shd->hqs', chosen, keys, precision=highest) * scale
            scores = jnp.where(key_live[None, None, :], scores, masked_score)
            weights = softmax_rows(scores).astype(jnp.bfloat16)
            return jnp.einsum('hqs,shd->qhd', widen(weights), values).astype(jnp.bfloat16)
        context = lax.map(query_group, queries).reshape(ROWS, E)
        late = stream + jnp.dot(context, item_out, preferred_element_type=jnp.float32)
        normed_late = layer_norm(late, norm_gain[2]).astype(jnp.bfloat16)
        hidden = jax.nn.gelu(jnp.dot(normed_late, mlp_in, preferred_element_type=jnp.float32), approximate=False).astype(jnp.bfloat16)
        return late + jnp.dot(hidden, mlp_out, preferred_element_type=jnp.float32)
    updated = lax.map(item_feature, jnp.transpose(cells_mid, (1, 0, 2)))
    return jnp.transpose(updated, (1, 0, 2))
```

```python
import math

import jax
import jax.numpy as jnp
from jax import lax
from jax.experimental import pallas as pl
from jax.experimental.pallas import tpu as pltpu
from jax.sharding import PartitionSpec as P

HEADS = 6
ROW = "row"
GRP_ROW = ("grp", "row")
f32 = jnp.float32
bf16 = jnp.bfloat16

norm_floor = 0.25
masked_score = -1e30


def nn(a, b):
    return lax.dot_general(a, b, (((1,), (0,)), ((), ())), preferred_element_type=f32)


def nt(a, b):
    return lax.dot_general(a, b, (((1,), (1,)), ((), ())), preferred_element_type=f32)


def tn(a, b):
    return lax.dot_general(a, b, (((0,), (0,)), ((), ())), preferred_element_type=f32)


def iota(shape, dim):
    return lax.broadcasted_iota(jnp.int32, shape, dim)


def onehot(mask):
    return jnp.where(mask, 1.0, 0.0).astype(bf16)


def layer_norm(v, gain):
    width = v.shape[-1]
    mean = jnp.sum(v, axis=-1, keepdims=True) * (1.0 / width)
    c = v - mean
    var = jnp.sum(c * c, axis=-1, keepdims=True) * (1.0 / width)
    return c * lax.rsqrt(var + norm_floor) * gain


def flipped(w):
    n = w.shape[0]
    eye = onehot(iota((n, n), 0) == iota((n, n), 1))
    return nt(eye, w).astype(bf16)


def spread_keys(w, head):
    n = w.shape[0]
    shape = (n, HEADS * 128)
    col = iota(shape, 1)
    lane = col & 127
    place = onehot((iota(shape, 0) == (col >> 7) * head + (lane & (head - 1))) & (lane < 3 * head))
    return nn(w, place).astype(bf16)


def prepare_weights(qkv, wq, wk, wv, head):
    wq[...] = flipped(qkv[0])
    wk[...] = spread_keys(qkv[1], head)
    wv[...] = flipped(qkv[2])


def fill_constant_rows(qs, vs, head):
    for h in range(HEADS):
        cols = qs.shape[-1]
        one_row = onehot(iota((head, cols), 0) == 0)
        qs[h, 3 * head : 4 * head, :] = one_row
        vs[h, head : head + 16, :] = jnp.ones((16, cols), bf16)


def project(x, bias, rows, wq, wk, wv, qs, ks, vs, head):
    scale = (1.0 / math.sqrt(head)) * math.log2(math.e)
    q = nt(wq[...], x) * scale
    qh = q.astype(bf16)
    ql = (q - qh.astype(f32)).astype(bf16)
    v = nt(wv[...], x).astype(bf16)
    for h in range(HEADS):
        mine = slice(h * head, (h + 1) * head)
        qs[h, 0:head, rows] = qh[mine]
        qs[h, head : 2 * head, rows] = ql[mine]
        qs[h, 2 * head : 3 * head, rows] = qh[mine]
        vs[h, 0:head, rows] = v[mine]
    lane = iota((x.shape[0], 128), 1)
    for h in range(HEADS):
        k = nn(x, wk[:, h * 128 : (h + 1) * 128])
        kh = k.astype(bf16).astype(f32)
        kl = k - kh
        packed = jnp.where(lane < 2 * head, kh, jnp.where(lane < 3 * head, kl, bias))
        ks[rows, h * 128 : (h + 1) * 128] = packed.astype(bf16)


def pack_maps(tokens, inner_rows, peers):
    rows = peers * (inner_rows + inner_rows // 2)
    shape = (rows, tokens)
    return iota(shape, 0), iota(shape, 1)


def front_kernel(present, cells, gain, qkv, wout, mid, send, xn, qs, ks, vs, ctx, wq, wk, wv):
    tokens, width = cells.shape
    head = width // HEADS
    feats = present.shape[-1]
    rows = tokens // feats
    prepare_weights(qkv, wq, wk, wv, head)
    fill_constant_rows(qs, vs, head)
    g0 = gain[0:1, :]
    for r in range(rows):
        at = slice(r * feats, (r + 1) * feats)
        xn[at, :] = layer_norm(cells[at, :], g0).astype(bf16)
    eye = iota((feats, feats), 0) == iota((feats, feats), 1)
    absent = jnp.where(present[...] > 0, 0.0, masked_score)
    bias = jnp.sum(jnp.where(eye, absent, 0.0), axis=1, keepdims=True)
    bias = jnp.concatenate([bias, bias], axis=0)
    step = 2 * feats
    for c in range(tokens // step):
        at = slice(c * step, (c + 1) * step)
        project(xn[at, :], bias, at, wq, wk, wv, qs, ks, vs, head)
    for r in range(rows):
        at = slice(r * feats, (r + 1) * feats)
        scores = [nn(ks[at, h * 128 : (h + 1) * 128], qs[h, :, at]) for h in range(HEADS)]
        weights = []
        for s in scores:
            top = jnp.max(s, axis=0, keepdims=True)
            weights.append(jnp.exp2(s - top).astype(bf16))
        for h in range(HEADS):
            o = nn(vs[h, :, at], weights[h])
            ctx[h * head : (h + 1) * head, at] = (o[0:head] * (1.0 / o[head : head + 1])).astype(bf16)
    g1 = gain[1:2, :]
    for r in range(rows):
        at = slice(r * feats, (r + 1) * feats)
        m = cells[at, :] + tn(ctx[:, at], wout[...])
        mid[at, :] = m
        xn[at, :] = layer_norm(m, g1).astype(bf16)
    o, t = pack_maps(rows * 16, rows, 16)
    f, r = t & 15, t >> 4
    base = f * 12
    low = onehot(o == base + r)
    first = onehot((o == base + 8 + (r & 3)) & (r < 4))
    second = onehot((o == base + 8 + (r & 3)) & (r >= 4))
    out_rows = o.shape[0]
    lane = iota((out_rows, 128), 1)
    for b in range(feats // 16):
        x = jnp.concatenate([xn[k * feats + b * 16 : k * feats + b * 16 + 16, :] for k in range(rows)], axis=0)
        tail = x[:, 128:width]
        tails = jnp.concatenate([tail, tail], axis=1)
        out = nn(low, x[:, 0:128]) + jnp.where(lane < 64, nn(first, tails), nn(second, tails))
        send[b * out_rows : (b + 1) * out_rows, :] = out.astype(bf16)


def rows_kernel(n_train, got, qkv, send, xn, qs, ks, vs, ctx, wq, wk, wv):
    width = qkv.shape[-1]
    head = width // HEADS
    total = xn.shape[0]
    prepare_weights(qkv, wq, wk, wv, head)
    fill_constant_rows(qs, vs, head)
    t, p = iota((128, 192), 0), iota((128, 192), 1)
    low = onehot(p == (t >> 3) * 12 + (t & 7))
    high = onehot(p == (t >> 3) * 12 + 8 + (t & 3))
    early = (iota((128, 64), 0) & 7) < 4
    for b in range(total // 128):
        a = got[b * 192 : (b + 1) * 192, :]
        hi = nn(high, a)
        xn[b * 128 : (b + 1) * 128, 0:128] = nn(low, a).astype(bf16)
        xn[b * 128 : (b + 1) * 128, 128:width] = jnp.where(early, hi[:, 0:64], hi[:, 64:128]).astype(bf16)
    live = n_train[0]
    step = 256
    for c in range(total // step):
        at = slice(c * step, (c + 1) * step)
        bias = jnp.where(iota((step, 1), 0) + c * step < live, 0.0, masked_score)
        project(xn[at, :], bias, at, wq, wk, wv, qs, ks, vs, head)

    def query_tile(j, carry):
        cols = pl.ds(pl.multiple_of(j * 256, 256), 256)

        def score(h):
            return nn(ks[:, h * 128 : (h + 1) * 128], qs[h, :, cols])

        s = score(0)
        for h in range(HEADS):
            ahead = score(h + 1) if h + 1 < HEADS else None
            top = jnp.max(s, axis=0, keepdims=True)
            w = jnp.exp2(s - top).astype(bf16)
            o = nn(vs[h], w)
            ctx[h * head : (h + 1) * head, cols] = (o[0:head] * (1.0 / o[head : head + 1])).astype(bf16)
            s = ahead
        return carry

    lax.fori_loop(0, total // 256, query_tile, 0)
    o, q = iota((192, 128), 0), iota((192, 128), 1)
    base, r = (q >> 3) * 12, q & 7
    low = onehot(o == base + r)
    first = onehot((o == base + 8 + (r & 3)) & (r < 4))
    second = onehot((o == base + 8 + (r & 3)) & (r >= 4))
    lane = iota((192, 128), 1)
    for b in range(total // 128):
        at = slice(b * 128, (b + 1) * 128)
        tail = ctx[128:width, at]
        tails = jnp.concatenate([tail, tail], axis=0)
        out = nt(low, ctx[0:128, at]) + jnp.where(lane < 64, nt(first, tails), nt(second, tails))
        send[b * 192 : (b + 1) * 192, :] = out.astype(bf16)


def tail_kernel(got, mid, gain, wout, w_in, w_out, result, ctx):
    tokens, width = mid.shape
    feats = tokens // 8
    t, p = iota((128, 192), 0), iota((128, 192), 1)
    low = onehot(p == (t & 15) * 12 + (t >> 4))
    high = onehot(p == (t & 15) * 12 + 8 + ((t >> 4) & 3))
    early = iota((128, 64), 0) < 64
    for b in range(feats // 16):
        a = got[b * 192 : (b + 1) * 192, :]
        hi = nn(high, a)
        lo = nn(low, a).astype(bf16)
        hi = jnp.where(early, hi[:, 0:64], hi[:, 64:128]).astype(bf16)
        for r in range(8):
            at = slice(r * feats + b * 16, r * feats + b * 16 + 16)
            ctx[at, 0:128] = lo[r * 16 : (r + 1) * 16]
            ctx[at, 128:width] = hi[r * 16 : (r + 1) * 16]
    g2 = gain[2:3, :]
    step = 256
    for c in range(tokens // step):
        at = slice(c * step, (c + 1) * step)
        late = mid[at, :] + nn(ctx[at, :], wout[...])
        n3 = layer_norm(late, g2).astype(bf16)
        z = nn(n3, w_in[...])
        hidden = (z * 0.5 * (1.0 + lax.erf(z * math.sqrt(0.5)))).astype(bf16)
        result[at, :] = late + nn(hidden, w_out[...])


def scratch(tokens, width):
    head = width // HEADS
    return [
        pltpu.VMEM((tokens, width), bf16),
        pltpu.VMEM((HEADS, 4 * head, tokens), bf16),
        pltpu.VMEM((tokens, HEADS * 128), bf16),
        pltpu.VMEM((HEADS, head + 16, tokens), bf16),
        pltpu.VMEM((width, tokens), bf16),
        pltpu.VMEM((width, width), bf16),
        pltpu.VMEM((width, HEADS * 128), bf16),
        pltpu.VMEM((width, width), bf16),
    ]


VMEM = pl.BlockSpec(memory_space=pltpu.VMEM)
SMEM = pl.BlockSpec(memory_space=pltpu.SMEM)


def front(present, cells, gain, qkv, wout):
    tokens, width = cells.shape
    return pl.pallas_call(
        front_kernel,
        out_shape=(
            jax.ShapeDtypeStruct((tokens, width), f32),
            jax.ShapeDtypeStruct((tokens * width // 128, 128), bf16),
        ),
        in_specs=[VMEM] * 5,
        out_specs=(VMEM, VMEM),
        scratch_shapes=scratch(tokens, width),
        name="front",
    )(present, cells, gain, qkv, wout)


def rows(n_train, got, qkv):
    width = qkv.shape[-1]
    tokens = got.shape[0] * 128 // width
    return pl.pallas_call(
        rows_kernel,
        out_shape=jax.ShapeDtypeStruct(got.shape, bf16),
        in_specs=[SMEM, VMEM, VMEM],
        out_specs=VMEM,
        scratch_shapes=scratch(tokens, width),
        name="rows",
    )(n_train, got, qkv)


def tail(got, mid, gain, wout, w_in, w_out):
    return pl.pallas_call(
        tail_kernel,
        out_shape=jax.ShapeDtypeStruct(mid.shape, f32),
        in_specs=[VMEM] * 6,
        out_specs=VMEM,
        scratch_shapes=[pltpu.VMEM(mid.shape, bf16)],
        name="tail",
    )(got, mid, gain, wout, w_in, w_out)


def exchanged(block):
    peers = lax.axis_size(ROW)
    tiles = block.reshape(peers, 3, 4, 128)
    return lax.all_to_all(tiles, ROW, 0, 0, tiled=True).reshape(block.shape)


def body(
    cells, n_train, present, norm_gain, feat_qkv, feat_out, item_qkv, item_out, mlp_in, mlp_out
):
    row_dev, feature_count, width = cells.shape
    flat = cells.reshape(row_dev * feature_count, width)
    mid, send = front(present.reshape(1, feature_count), flat, norm_gain, feat_qkv, feat_out)
    got = exchanged(send)
    back = rows(n_train, got, item_qkv)
    returned = exchanged(back)
    out = tail(returned, mid, norm_gain, item_out, mlp_in, mlp_out)
    return out.reshape(cells.shape)


def solution(mesh):
    return jax.shard_map(
        body,
        mesh=mesh,
        in_specs=(P(GRP_ROW, None, None), P("grp"), P("grp"), P(), P(), P(), P(), P(), P(), P()),
        out_specs=P(GRP_ROW, None, None),
        check_vma=False,
    )
```

```python
import math

import jax
import jax.numpy as jnp
from jax import lax
from jax.experimental import pallas as pl
from jax.experimental.pallas import tpu as pltpu
from jax.sharding import PartitionSpec as P

HEADS = 6
ROW = "row"
GRP_ROW = ("grp", "row")
f32 = jnp.float32
bf16 = jnp.bfloat16

norm_floor = 0.25
masked_score = -1e30


def nn(a, b):
    return lax.dot_general(a, b, (((1,), (0,)), ((), ())), preferred_element_type=f32)


def nt(a, b):
    return lax.dot_general(a, b, (((1,), (1,)), ((), ())), preferred_element_type=f32)


def tn(a, b):
    return lax.dot_general(a, b, (((0,), (0,)), ((), ())), preferred_element_type=f32)


def iota(shape, dim):
    return lax.broadcasted_iota(jnp.int32, shape, dim)


def onehot(mask):
    return jnp.where(mask, 1.0, 0.0).astype(bf16)


def layer_norm(v, gain):
    scale = 1.0 / v.shape[0]
    mean = jnp.sum(v, axis=0, keepdims=True) * scale
    c = v - mean
    var = jnp.sum(c * c, axis=0, keepdims=True) * scale
    return c * lax.rsqrt(var + norm_floor) * gain


def column(row):
    n = row.shape[-1]
    eye = iota((n, n), 0) == iota((n, n), 1)
    return jnp.sum(jnp.where(eye, row, 0.0), axis=1, keepdims=True)


def flipped(w):
    n = w.shape[0]
    eye = onehot(iota((n, n), 0) == iota((n, n), 1))
    return nt(eye, w).astype(bf16)


def spread_keys(w, head):
    n = w.shape[0]
    shape = (n, HEADS * 128)
    col = iota(shape, 1)
    lane = col & 127
    place = onehot((iota(shape, 0) == (col >> 7) * head + (lane & (head - 1))) & (lane < 3 * head))
    return nn(w, place).astype(bf16)


def prepare_weights(qkv, wq, wk, wv, head):
    wq[...] = flipped(qkv[0])
    wk[...] = spread_keys(qkv[1], head)
    wv[...] = flipped(qkv[2])


def fill_constant_rows(qs, vs, head):
    for h in range(HEADS):
        cols = qs.shape[-1]
        one_row = onehot(iota((head, cols), 0) == 0)
        qs[h, 3 * head : 4 * head, :] = one_row
        vs[h, head : head + 16, :] = jnp.ones((16, cols), bf16)


def project(xt, x, bias, rows, wq, wk, wv, qs, ks, vs, head):
    scale = (1.0 / math.sqrt(head)) * math.log2(math.e)
    q = (nn(wq[...], xt) if xt is not None else nt(wq[...], x)) * scale
    qh = q.astype(bf16)
    ql = (q - qh.astype(f32)).astype(bf16)
    v = (nn(wv[...], xt) if xt is not None else nt(wv[...], x)).astype(bf16)
    for h in range(HEADS):
        mine = slice(h * head, (h + 1) * head)
        qs[h, 0:head, rows] = qh[mine]
        qs[h, head : 2 * head, rows] = ql[mine]
        qs[h, 2 * head : 3 * head, rows] = qh[mine]
        vs[h, 0:head, rows] = v[mine]
    lane = iota((x.shape[0], 128), 1)
    for h in range(HEADS):
        k = nn(x, wk[:, h * 128 : (h + 1) * 128])
        kh = k.astype(bf16).astype(f32)
        kl = k - kh
        packed = jnp.where(lane < 2 * head, kh, jnp.where(lane < 3 * head, kl, bias))
        ks[rows, h * 128 : (h + 1) * 128] = packed.astype(bf16)


def front_kernel(present, cells, gain, qkv, wout, mid, send, xn, qs, ks, vs, ctx, wq, wk, wv):
    rows, width, feats = cells.shape
    head = width // HEADS
    prepare_weights(qkv, wq, wk, wv, head)
    wo = flipped(wout[...])
    fill_constant_rows(qs, vs, head)
    g0 = jnp.broadcast_to(column(gain[0:1, :]), (width, feats))
    g1 = jnp.broadcast_to(column(gain[1:2, :]), (width, feats))
    bias = column(jnp.where(present[...] > 0, 0.0, masked_score))
    bias = jnp.concatenate([bias, bias], axis=0)
    for c in range(rows // 2):
        xt = jnp.concatenate([layer_norm(cells[2 * c + k], g0).astype(bf16) for k in range(2)], axis=1)
        project(xt, xt.T, bias, slice(c * 2 * feats, (c + 1) * 2 * feats), wq, wk, wv, qs, ks, vs, head)
    for r in range(rows):
        at = slice(r * feats, (r + 1) * feats)
        scores = [nn(ks[at, h * 128 : (h + 1) * 128], qs[h, :, at]) for h in range(HEADS)]
        weights = []
        for s in scores:
            top = jnp.max(s, axis=0, keepdims=True)
            weights.append(jnp.exp2(s - top).astype(bf16))
        for h in range(HEADS):
            o = nn(vs[h, :, at], weights[h])
            ctx[h * head : (h + 1) * head, at] = (o[0:head] * (1.0 / o[head : head + 1])).astype(bf16)
    for c in range(rows // 2):
        both = nn(wo, ctx[:, c * 2 * feats : (c + 1) * 2 * feats])
        for k in range(2):
            r = 2 * c + k
            m = cells[r] + both[:, k * feats : (k + 1) * feats]
            mid[r] = m
            xn[r * feats : (r + 1) * feats, :] = layer_norm(m, g1).astype(bf16).T
    shape = (192, rows * 16)
    o, t = iota(shape, 0), iota(shape, 1)
    f, r = t & 15, t >> 4
    base = f * 12
    low = onehot(o == base + r)
    first = onehot((o == base + 8 + (r & 3)) & (r < 4))
    second = onehot((o == base + 8 + (r & 3)) & (r >= 4))
    lane = iota((192, 128), 1)
    for b in range(feats // 16):
        x = jnp.concatenate([xn[k * feats + b * 16 : k * feats + b * 16 + 16, :] for k in range(rows)], axis=0)
        tail = x[:, 128:width]
        tails = jnp.concatenate([tail, tail], axis=1)
        out = nn(low, x[:, 0:128]) + jnp.where(lane < 64, nn(first, tails), nn(second, tails))
        send[b * 192 : (b + 1) * 192, :] = out.astype(bf16)


def rows_kernel(n_train, got, qkv, send, xn, qs, ks, vs, ctx, wq, wk, wv):
    width = qkv.shape[-1]
    head = width // HEADS
    total = xn.shape[0]
    prepare_weights(qkv, wq, wk, wv, head)
    fill_constant_rows(qs, vs, head)
    t, p = iota((128, 192), 0), iota((128, 192), 1)
    low = onehot(p == (t >> 3) * 12 + (t & 7))
    high = onehot(p == (t >> 3) * 12 + 8 + (t & 3))
    early = (iota((128, 64), 0) & 7) < 4
    for b in range(total // 128):
        a = got[b * 192 : (b + 1) * 192, :]
        hi = nn(high, a)
        xn[b * 128 : (b + 1) * 128, 0:128] = nn(low, a).astype(bf16)
        xn[b * 128 : (b + 1) * 128, 128:width] = jnp.where(early, hi[:, 0:64], hi[:, 64:128]).astype(bf16)
    live = n_train[0]
    step = 256
    for c in range(total // step):
        at = slice(c * step, (c + 1) * step)
        bias = jnp.where(iota((step, 1), 0) + c * step < live, 0.0, masked_score)
        project(None, xn[at, :], bias, at, wq, wk, wv, qs, ks, vs, head)

    def query_tile(j, carry):
        cols = pl.ds(pl.multiple_of(j * 256, 256), 256)

        def score(h):
            return nn(ks[:, h * 128 : (h + 1) * 128], qs[h, :, cols])

        s = score(0)
        for h in range(HEADS):
            ahead = score(h + 1) if h + 1 < HEADS else None
            top = jnp.max(s, axis=0, keepdims=True)
            w = jnp.exp2(s - top).astype(bf16)
            o = nn(vs[h], w)
            ctx[h * head : (h + 1) * head, cols] = (o[0:head] * (1.0 / o[head : head + 1])).astype(bf16)
            s = ahead
        return carry

    lax.fori_loop(0, total // 256, query_tile, 0)
    o, q = iota((192, 128), 0), iota((192, 128), 1)
    base, r = (q >> 3) * 12, q & 7
    low = onehot(o == base + r)
    first = onehot((o == base + 8 + (r & 3)) & (r < 4))
    second = onehot((o == base + 8 + (r & 3)) & (r >= 4))
    lane = iota((192, 128), 1)
    for b in range(total // 128):
        at = slice(b * 128, (b + 1) * 128)
        tail = ctx[128:width, at]
        tails = jnp.concatenate([tail, tail], axis=0)
        out = nt(low, ctx[0:128, at]) + jnp.where(lane < 64, nt(first, tails), nt(second, tails))
        send[b * 192 : (b + 1) * 192, :] = out.astype(bf16)


def tail_kernel(got, mid, gain, wout, w_in, w_out, result, ctx):
    rows, width, feats = mid.shape
    t, p = iota((128, 192), 0), iota((128, 192), 1)
    low = onehot(p == (t & 15) * 12 + (t >> 4))
    high = onehot(p == (t & 15) * 12 + 8 + ((t >> 4) & 3))
    early = iota((128, 64), 0) < 64
    wo = flipped(wout[...])
    wi = w_in[...].T
    for b in range(feats // 16):
        a = got[b * 192 : (b + 1) * 192, :]
        hi = nn(high, a)
        lo = nn(low, a).astype(bf16)
        hi = jnp.where(early, hi[:, 0:64], hi[:, 64:128]).astype(bf16)
        for r in range(rows):
            at = slice(r * feats + b * 16, r * feats + b * 16 + 16)
            ctx[at, 0:128] = lo[r * 16 : (r + 1) * 16]
            ctx[at, 128:width] = hi[r * 16 : (r + 1) * 16]
    g2 = jnp.broadcast_to(column(gain[2:3, :]), (width, 2 * feats))
    for c in range(rows // 2):
        old = jnp.concatenate([mid[2 * c], mid[2 * c + 1]], axis=1)
        late = old + nt(wo, ctx[c * 2 * feats : (c + 1) * 2 * feats, :])
        n3 = layer_norm(late, g2).astype(bf16)
        z = nn(wi, n3)
        hidden = (z * 0.5 * (1.0 + lax.erf(z * math.sqrt(0.5)))).astype(bf16)
        out = late + nn(w_out[...], hidden)
        result[2 * c] = out[:, 0:feats]
        result[2 * c + 1] = out[:, feats : 2 * feats]


def scratch(tokens, width):
    head = width // HEADS
    return [
        pltpu.VMEM((tokens, width), bf16),
        pltpu.VMEM((HEADS, 4 * head, tokens), bf16),
        pltpu.VMEM((tokens, HEADS * 128), bf16),
        pltpu.VMEM((HEADS, head + 16, tokens), bf16),
        pltpu.VMEM((width, tokens), bf16),
        pltpu.VMEM((width, width), bf16),
        pltpu.VMEM((width, HEADS * 128), bf16),
        pltpu.VMEM((width, width), bf16),
    ]


VMEM = pl.BlockSpec(memory_space=pltpu.VMEM)
SMEM = pl.BlockSpec(memory_space=pltpu.SMEM)


def front(present, cells, gain, qkv, wout):
    rows, width, feats = cells.shape
    tokens = rows * feats
    return pl.pallas_call(
        front_kernel,
        out_shape=(
            jax.ShapeDtypeStruct(cells.shape, f32),
            jax.ShapeDtypeStruct((tokens * width // 128, 128), bf16),
        ),
        in_specs=[VMEM] * 5,
        out_specs=(VMEM, VMEM),
        scratch_shapes=scratch(tokens, width),
        name="front",
    )(present, cells, gain, qkv, wout)


def rows(n_train, got, qkv):
    width = qkv.shape[-1]
    tokens = got.shape[0] * 128 // width
    return pl.pallas_call(
        rows_kernel,
        out_shape=jax.ShapeDtypeStruct(got.shape, bf16),
        in_specs=[SMEM, VMEM, VMEM],
        out_specs=VMEM,
        scratch_shapes=scratch(tokens, width),
        name="rows",
    )(n_train, got, qkv)


def tail(got, mid, gain, wout, w_in, w_out):
    rows, width, feats = mid.shape
    return pl.pallas_call(
        tail_kernel,
        out_shape=jax.ShapeDtypeStruct(mid.shape, f32),
        in_specs=[VMEM] * 6,
        out_specs=VMEM,
        scratch_shapes=[pltpu.VMEM((rows * feats, width), bf16)],
        name="tail",
    )(got, mid, gain, wout, w_in, w_out)


def exchanged(block):
    peers = lax.axis_size(ROW)
    tiles = block.reshape(peers, 3, 4, 128)
    return lax.all_to_all(tiles, ROW, 0, 0, tiled=True).reshape(block.shape)


def body(
    cells, n_train, present, norm_gain, feat_qkv, feat_out, item_qkv, item_out, mlp_in, mlp_out
):
    stood = jnp.transpose(cells, (0, 2, 1))
    mid, send = front(present.reshape(1, -1), stood, norm_gain, feat_qkv, feat_out)
    got = exchanged(send)
    back = rows(n_train, got, item_qkv)
    returned = exchanged(back)
    out = tail(returned, mid, norm_gain, item_out, mlp_in, jnp.transpose(mlp_out))
    return jnp.transpose(out, (0, 2, 1))


def solution(mesh):
    return jax.shard_map(
        body,
        mesh=mesh,
        in_specs=(P(GRP_ROW, None, None), P("grp"), P("grp"), P(), P(), P(), P(), P(), P(), P()),
        out_specs=P(GRP_ROW, None, None),
        check_vma=False,
    )
```

```python
import math

import jax
import jax.numpy as jnp
from jax import lax
from jax.experimental import pallas as pl
from jax.experimental.pallas import tpu as pltpu
from jax.sharding import PartitionSpec as P

HEADS = 6
ROW = "row"
GRP_ROW = ("grp", "row")
f32 = jnp.float32
bf16 = jnp.bfloat16

norm_floor = 0.25
masked_score = -1e30


def nn(a, b):
    return lax.dot_general(a, b, (((1,), (0,)), ((), ())), preferred_element_type=f32)


def nt(a, b):
    return lax.dot_general(a, b, (((1,), (1,)), ((), ())), preferred_element_type=f32)


def tn(a, b):
    return lax.dot_general(a, b, (((0,), (0,)), ((), ())), preferred_element_type=f32)


def iota(shape, dim):
    return lax.broadcasted_iota(jnp.int32, shape, dim)


def onehot(mask):
    return jnp.where(mask, 1.0, 0.0).astype(bf16)


def layer_norm(v, gain):
    scale = 1.0 / v.shape[0]
    mean = jnp.sum(v, axis=0, keepdims=True) * scale
    c = v - mean
    var = jnp.sum(c * c, axis=0, keepdims=True) * scale
    return c * lax.rsqrt(var + norm_floor) * gain


def column(row):
    n = row.shape[-1]
    eye = iota((n, n), 0) == iota((n, n), 1)
    return jnp.sum(jnp.where(eye, row, 0.0), axis=1, keepdims=True)


def flipped(w):
    n = w.shape[0]
    eye = onehot(iota((n, n), 0) == iota((n, n), 1))
    return nt(eye, w).astype(bf16)


def prepare_weights(qkv, wt):
    width = qkv.shape[-1]
    for c in range(3):
        wt[c * width : (c + 1) * width, :] = flipped(qkv[c])


def fill_constant_rows(qs, vs, head):
    cols = qs.shape[-1]
    one_row = onehot(iota((head, cols), 0) == 0)
    for h in range(HEADS):
        qs[h, 3 * head : 4 * head, :] = one_row
        vs[h, head : head + 16, :] = jnp.ones((16, cols), bf16)


def split(v):
    hi = v.astype(bf16)
    return hi, (v - hi.astype(f32)).astype(bf16)


def project(triple, bias, rows, qs, ks, vs, head):
    width = triple.shape[0] // 3
    scale = (1.0 / math.sqrt(head)) * math.log2(math.e)
    qh, ql = split(triple[0:width] * scale)
    kh, kl = split(triple[width : 2 * width])
    v = triple[2 * width : 3 * width].astype(bf16)
    shape = (head, triple.shape[1])
    last = jnp.where(iota(shape, 0) == 0, bias, 0.0).astype(bf16)
    for h in range(HEADS):
        mine = slice(h * head, (h + 1) * head)
        qs[h, 0:head, rows] = qh[mine]
        qs[h, head : 2 * head, rows] = ql[mine]
        qs[h, 2 * head : 3 * head, rows] = qh[mine]
        vs[h, 0:head, rows] = v[mine]
        stack = jnp.concatenate([kh[mine], kh[mine], kl[mine], last], axis=0)
        ks[rows, h * 128 : (h + 1) * 128] = stack.T


def front_kernel(present, cells, gain, qkv, wout, mid, send, xn, qs, ks, vs, ctx, wt, raw, sems):
    rows, width, feats = cells.shape
    head = width // HEADS
    copies = [pltpu.make_async_copy(cells.at[r], raw.at[r], sems.at[r]) for r in range(rows)]
    for c in copies:
        c.start()
    prepare_weights(qkv, wt)
    wo = flipped(wout[...])
    fill_constant_rows(qs, vs, head)
    g0 = jnp.broadcast_to(column(gain[0:1, :]), (width, feats))
    g1 = jnp.broadcast_to(column(gain[1:2, :]), (width, feats))
    bias = jnp.where(present[...] > 0, 0.0, masked_score)
    bias = jnp.concatenate([bias, bias], axis=1)
    for c in range(rows // 2):
        copies[2 * c].wait()
        copies[2 * c + 1].wait()
        xt = jnp.concatenate([layer_norm(raw[2 * c + k], g0).astype(bf16) for k in range(2)], axis=1)
        project(nn(wt[...], xt), bias, slice(c * 2 * feats, (c + 1) * 2 * feats), qs, ks, vs, head)
    for r in range(rows):
        at = slice(r * feats, (r + 1) * feats)
        scores = [nn(ks[at, h * 128 : (h + 1) * 128], qs[h, :, at]) for h in range(HEADS)]
        weights = []
        for s in scores:
            top = jnp.max(s, axis=0, keepdims=True)
            weights.append(jnp.exp2(s - top).astype(bf16))
        for h in range(HEADS):
            o = nn(vs[h, :, at], weights[h])
            ctx[h * head : (h + 1) * head, at] = (o[0:head] * (1.0 / o[head : head + 1])).astype(bf16)
    for c in range(rows // 2):
        both = nn(wo, ctx[:, c * 2 * feats : (c + 1) * 2 * feats])
        for k in range(2):
            r = 2 * c + k
            m = raw[r] + both[:, k * feats : (k + 1) * feats]
            mid[r] = m
            xn[r * feats : (r + 1) * feats, :] = layer_norm(m, g1).astype(bf16).T
    shape = (192, rows * 16)
    o, t = iota(shape, 0), iota(shape, 1)
    f, r = t & 15, t >> 4
    base = f * 12
    low = onehot(o == base + r)
    first = onehot((o == base + 8 + (r & 3)) & (r < 4))
    second = onehot((o == base + 8 + (r & 3)) & (r >= 4))
    lane = iota((192, 128), 1)
    for b in range(feats // 16):
        x = jnp.concatenate([xn[k * feats + b * 16 : k * feats + b * 16 + 16, :] for k in range(rows)], axis=0)
        tail = x[:, 128:width]
        tails = jnp.concatenate([tail, tail], axis=1)
        out = nn(low, x[:, 0:128]) + jnp.where(lane < 64, nn(first, tails), nn(second, tails))
        send[b * 192 : (b + 1) * 192, :] = out.astype(bf16)


def rows_kernel(n_train, got, qkv, send, xn, qs, ks, vs, ctx, wt, sbuf):
    width = qkv.shape[-1]
    head = width // HEADS
    total = xn.shape[0]
    prepare_weights(qkv, wt)
    fill_constant_rows(qs, vs, head)
    t, p = iota((128, 192), 0), iota((128, 192), 1)
    low = onehot(p == (t >> 3) * 12 + (t & 7))
    high = onehot(p == (t >> 3) * 12 + 8 + (t & 3))
    early = (iota((128, 64), 0) & 7) < 4
    for b in range(total // 128):
        a = got[b * 192 : (b + 1) * 192, :]
        hi = nn(high, a)
        xn[b * 128 : (b + 1) * 128, 0:128] = nn(low, a).astype(bf16)
        xn[b * 128 : (b + 1) * 128, 128:width] = jnp.where(early, hi[:, 0:64], hi[:, 64:128]).astype(bf16)
    live = n_train[0]
    step = 256
    for c in range(total // step):
        at = slice(c * step, (c + 1) * step)
        bias = jnp.where(iota((1, step), 1) + c * step < live, 0.0, masked_score)
        project(nt(wt[...], xn[at, :]), bias, at, qs, ks, vs, head)

    tiles = total // 256
    blocks = total // 256

    def score(h, cols, b):
        s = nn(ks[b * 256 : (b + 1) * 256, h * 128 : (h + 1) * 128], qs[h, :, cols])
        sbuf[h % 2, b * 256 : (b + 1) * 256, :] = s
        return jnp.max(s.reshape(32, 8, 256), axis=0)

    def columns(j):
        return pl.ds(pl.multiple_of(j * 256, 256), 256)

    peak = score(0, slice(0, 256), 0)
    for b in range(1, blocks):
        peak = jnp.maximum(peak, score(0, slice(0, 256), b))

    def query_tile(j, peak):
        cols = columns(j)
        after = columns(jnp.minimum(j + 1, tiles - 1))
        for h in range(HEADS):
            top = jnp.max(peak, axis=0, keepdims=True)
            o = None
            peak = None
            for b in range(blocks):
                ahead = score(h + 1, cols, b) if h + 1 < HEADS else score(0, after, b)
                peak = ahead if peak is None else jnp.maximum(peak, ahead)
                w = jnp.exp2(sbuf[h % 2, b * 256 : (b + 1) * 256, :] - top).astype(bf16)
                part = nn(vs[h, :, b * 256 : (b + 1) * 256], w)
                o = part if o is None else o + part
            ctx[h * head : (h + 1) * head, cols] = (o[0:head] * (1.0 / o[head : head + 1])).astype(bf16)
        return peak

    lax.fori_loop(0, tiles, query_tile, peak)
    o, q = iota((192, 128), 0), iota((192, 128), 1)
    base, r = (q >> 3) * 12, q & 7
    low = onehot(o == base + r)
    first = onehot((o == base + 8 + (r & 3)) & (r < 4))
    second = onehot((o == base + 8 + (r & 3)) & (r >= 4))
    lane = iota((192, 128), 1)
    for b in range(total // 128):
        at = slice(b * 128, (b + 1) * 128)
        tail = ctx[128:width, at]
        tails = jnp.concatenate([tail, tail], axis=0)
        out = nt(low, ctx[0:128, at]) + jnp.where(lane < 64, nt(first, tails), nt(second, tails))
        send[b * 192 : (b + 1) * 192, :] = out.astype(bf16)


def tail_kernel(got, mid, gain, wout, w_in, w_out, result, ctx, out_buf, sems):
    rows, width, feats = mid.shape
    t, p = iota((128, 192), 0), iota((128, 192), 1)
    low = onehot(p == (t & 15) * 12 + (t >> 4))
    high = onehot(p == (t & 15) * 12 + 8 + ((t >> 4) & 3))
    early = iota((128, 64), 0) < 64
    wo = flipped(wout[...])
    wi = w_in[...].T
    for b in range(feats // 16):
        a = got[b * 192 : (b + 1) * 192, :]
        hi = nn(high, a)
        lo = nn(low, a).astype(bf16)
        hi = jnp.where(early, hi[:, 0:64], hi[:, 64:128]).astype(bf16)
        for r in range(rows):
            at = slice(r * feats + b * 16, r * feats + b * 16 + 16)
            ctx[at, 0:128] = lo[r * 16 : (r + 1) * 16]
            ctx[at, 128:width] = hi[r * 16 : (r + 1) * 16]
    g2 = jnp.broadcast_to(column(gain[2:3, :]), (width, 2 * feats))
    sent = []
    for c in range(rows // 2):
        old = jnp.concatenate([mid[2 * c], mid[2 * c + 1]], axis=1)
        late = old + nt(wo, ctx[c * 2 * feats : (c + 1) * 2 * feats, :])
        n3 = layer_norm(late, g2).astype(bf16)
        z = nn(wi, n3)
        hidden = (z * 0.5 * (1.0 + lax.erf(z * math.sqrt(0.5)))).astype(bf16)
        out = late + nn(w_out[...], hidden)
        for k in range(2):
            out_buf[2 * c + k] = out[:, k * feats : (k + 1) * feats]
            sent.append(pltpu.make_async_copy(out_buf.at[2 * c + k], result.at[2 * c + k], sems.at[2 * c + k]))
            sent[-1].start()
    for s in sent:
        s.wait()


def scratch(tokens, width):
    head = width // HEADS
    return [
        pltpu.VMEM((tokens, width), bf16),
        pltpu.VMEM((HEADS, 4 * head, tokens), bf16),
        pltpu.VMEM((tokens, HEADS * 128), bf16),
        pltpu.VMEM((HEADS, head + 16, tokens), bf16),
        pltpu.VMEM((width, tokens), bf16),
        pltpu.VMEM((3 * width, width), bf16),
    ]


VMEM = pl.BlockSpec(memory_space=pltpu.VMEM)
SMEM = pl.BlockSpec(memory_space=pltpu.SMEM)
ANY = pl.BlockSpec(memory_space=pl.ANY)


def near(x):
    return pltpu.with_memory_space_constraint(x, pltpu.VMEM)


def front(present, cells, gain, qkv, wout):
    rows, width, feats = cells.shape
    tokens = rows * feats
    return pl.pallas_call(
        front_kernel,
        out_shape=(
            pltpu.VMEM(cells.shape, f32),
            pltpu.VMEM((tokens * width // 128, 128), bf16),
        ),
        in_specs=[VMEM, ANY, VMEM, VMEM, VMEM],
        out_specs=(VMEM, VMEM),
        scratch_shapes=[*scratch(tokens, width), pltpu.VMEM(cells.shape, f32), pltpu.SemaphoreType.DMA((rows,))],
        name="front",
    )(present, cells, gain, qkv, wout)


def rows(n_train, got, qkv):
    width = qkv.shape[-1]
    tokens = got.shape[0] * 128 // width
    return pl.pallas_call(
        rows_kernel,
        out_shape=pltpu.VMEM(got.shape, bf16),
        in_specs=[SMEM, VMEM, VMEM],
        out_specs=VMEM,
        scratch_shapes=[*scratch(tokens, width), pltpu.VMEM((2, tokens, 256), f32)],
        name="rows",
    )(n_train, near(got), near(qkv))


def tail(got, mid, gain, wout, w_in, w_out):
    rows, width, feats = mid.shape
    return pl.pallas_call(
        tail_kernel,
        out_shape=jax.ShapeDtypeStruct(mid.shape, f32),
        in_specs=[VMEM] * 6,
        out_specs=ANY,
        scratch_shapes=[
            pltpu.VMEM((rows * feats, width), bf16),
            pltpu.VMEM(mid.shape, f32),
            pltpu.SemaphoreType.DMA((rows,)),
        ],
        name="tail",
    )(near(got), near(mid), near(gain), near(wout), near(w_in), near(w_out))


def exchanged(block):
    peers = lax.axis_size(ROW)
    tiles = block.reshape(peers, 3, 4, 128)
    return lax.all_to_all(tiles, ROW, 0, 0, tiled=True).reshape(block.shape)


def body(
    cells, n_train, present, norm_gain, feat_qkv, feat_out, item_qkv, item_out, mlp_in, mlp_out
):
    stood = jnp.transpose(cells, (0, 2, 1))
    mid, send = front(present.reshape(1, -1), stood, norm_gain, feat_qkv, feat_out)
    got = exchanged(send)
    back = rows(n_train, got, item_qkv)
    returned = exchanged(back)
    out = tail(returned, mid, norm_gain, item_out, mlp_in, jnp.transpose(mlp_out))
    return jnp.transpose(out, (0, 2, 1))


def solution(mesh):
    return jax.shard_map(
        body,
        mesh=mesh,
        in_specs=(P(GRP_ROW, None, None), P("grp"), P("grp"), P(), P(), P(), P(), P(), P(), P()),
        out_specs=P(GRP_ROW, None, None),
        check_vma=False,
    )
```

```python
import math

import jax
import jax.numpy as jnp
from jax import lax
from jax.experimental import pallas as pl
from jax.experimental.pallas import tpu as pltpu
from jax.sharding import PartitionSpec as P

HEADS = 6
ROW = "row"
GRP_ROW = ("grp", "row")
f32 = jnp.float32
bf16 = jnp.bfloat16

norm_floor = 0.25
masked_score = -1e30


def nn(a, b):
    return lax.dot_general(a, b, (((1,), (0,)), ((), ())), preferred_element_type=f32)


def nt(a, b):
    return lax.dot_general(a, b, (((1,), (1,)), ((), ())), preferred_element_type=f32)


def tn(a, b):
    return lax.dot_general(a, b, (((0,), (0,)), ((), ())), preferred_element_type=f32)


def iota(shape, dim):
    return lax.broadcasted_iota(jnp.int32, shape, dim)


def onehot(mask):
    return jnp.where(mask, 1.0, 0.0).astype(bf16)


def layer_norm(v, gain):
    scale = 1.0 / v.shape[0]
    mean = jnp.sum(v, axis=0, keepdims=True) * scale
    c = v - mean
    var = jnp.sum(c * c, axis=0, keepdims=True) * scale
    return c * lax.rsqrt(var + norm_floor) * gain


def column(row):
    n = row.shape[-1]
    eye = iota((n, n), 0) == iota((n, n), 1)
    return jnp.sum(jnp.where(eye, row, 0.0), axis=1, keepdims=True)


def prepare_weights(qkv, wt):
    width = qkv.shape[-1]
    for c in range(3):
        wt[c * width : (c + 1) * width, :] = qkv[c].T


def fill_constant_rows(qs, vs, head):
    cols = qs.shape[-1]
    one_row = onehot(iota((head, cols), 0) == 0)
    for h in range(HEADS):
        qs[h, 3 * head : 4 * head, :] = one_row
        vs[h, head : head + 16, :] = jnp.ones((16, cols), bf16)


def split(v):
    hi = v.astype(bf16)
    return hi, (v - hi.astype(f32)).astype(bf16)


def project(triple, bias, rows, qs, ks, vs, head):
    width = triple.shape[0] // 3
    scale = (1.0 / math.sqrt(head)) * math.log2(math.e)
    qh, ql = split(triple[0:width] * scale)
    kh, kl = split(triple[width : 2 * width])
    v = triple[2 * width : 3 * width].astype(bf16)
    shape = (head, triple.shape[1])
    last = jnp.where(iota(shape, 0) == 0, bias, 0.0).astype(bf16)
    for h in range(HEADS):
        mine = slice(h * head, (h + 1) * head)
        qs[h, 0:head, rows] = qh[mine]
        qs[h, head : 2 * head, rows] = ql[mine]
        qs[h, 2 * head : 3 * head, rows] = qh[mine]
        vs[h, 0:head, rows] = v[mine]
        stack = jnp.concatenate([kh[mine], kh[mine], kl[mine], last], axis=0)
        ks[rows, h * 128 : (h + 1) * 128] = stack.T


def front_kernel(
    present, cells, gain, qkv, wout, mid, send, raw, wq, wo, xn, qs, ks, vs, ctx, wt, cell_sems, sems
):
    rows, width, feats = cells.shape
    head = width // HEADS
    step = 2 * feats
    chunks = rows // 2
    copies = [pltpu.make_async_copy(cells.at[r], raw.at[r], cell_sems.at[r]) for r in range(rows)]
    first = pltpu.make_async_copy(qkv, wq, sems.at[0])
    second = pltpu.make_async_copy(wout, wo, sems.at[1])
    copies[0].start()
    copies[1].start()
    first.start()
    for c in copies[2:]:
        c.start()
    second.start()
    for p in range(HEADS // 2):
        for r in range(rows):
            qs[p, 0:128, r * step + feats : (r + 1) * step] = jnp.zeros((128, feats), bf16)
            qs[p, 128:256, r * step : r * step + feats] = jnp.zeros((128, feats), bf16)
            one_row = onehot(iota((head, feats), 0) == 0)
            qs[p, 3 * head : 4 * head, r * step : r * step + feats] = one_row
            qs[p, 7 * head : 8 * head, r * step + feats : (r + 1) * step] = one_row
    for h in range(HEADS):
        at = h * (head + 16) + head
        vs[at : at + 16, :] = jnp.ones((16, rows * feats), bf16)
    g0 = jnp.broadcast_to(column(gain[0:1, :]), (width, feats))
    g1 = jnp.broadcast_to(column(gain[1:2, :]), (width, feats))
    bias = jnp.where(present[...] > 0, 0.0, masked_score)
    bias = jnp.concatenate([bias, bias], axis=1)
    last = jnp.where(iota((head, step), 0) == 0, bias, 0.0).astype(bf16)
    first.wait()
    prepare_weights(wq, wt)
    scale = (1.0 / math.sqrt(head)) * math.log2(math.e)

    def normed(c):
        copies[2 * c].wait()
        copies[2 * c + 1].wait()
        return jnp.concatenate([layer_norm(raw[2 * c + k], g0).astype(bf16) for k in range(2)], axis=1)

    def place(c, triple):
        tok = slice(c * step, (c + 1) * step)
        qh, ql = split(triple[0:width] * scale)
        kh, kl = split(triple[width : 2 * width])
        v = triple[2 * width : 3 * width].astype(bf16)
        for h in range(HEADS):
            mine = slice(h * head, (h + 1) * head)
            vs[h * (head + 16) : h * (head + 16) + head, tok] = v[mine]
            up = (h % 2) * 128
            for k in range(2):
                col = (2 * c + k) * step + (h % 2) * feats
                part = slice(k * feats, (k + 1) * feats)
                qs[h // 2, up : up + head, col : col + feats] = qh[mine, part]
                qs[h // 2, up + head : up + 2 * head, col : col + feats] = ql[mine, part]
                qs[h // 2, up + 2 * head : up + 3 * head, col : col + feats] = qh[mine, part]
            ks[tok, h * 128 : (h + 1) * 128] = jnp.concatenate([kh[mine], kh[mine], kl[mine], last], axis=0).T

    xt = normed(0)
    triple = nn(wt[...], xt)
    for c in range(chunks):
        if c + 1 < chunks:
            ahead = nn(wt[...], normed(c + 1))
        place(c, triple)
        triple = ahead

    def scores(r):
        at = slice(r * feats, (r + 1) * feats)
        return [nn(ks[at, p * 256 : (p + 1) * 256], qs[p, :, r * step : (r + 1) * step]) for p in range(HEADS // 2)]

    def attend(r, s):
        at = slice(r * feats, (r + 1) * feats)
        w = [jnp.exp2(x - jnp.max(x, axis=0, keepdims=True)).astype(bf16) for x in s]
        for p in range(HEADS // 2):
            o = nn(vs[p * 2 * (head + 16) : (p + 1) * 2 * (head + 16), at], w[p])
            for k in range(2):
                lane, row = slice(k * feats, (k + 1) * feats), k * (head + 16)
                h = 2 * p + k
                inverse = 1.0 / o[row + head : row + head + 1, lane]
                ctx[h * head : (h + 1) * head, at] = (o[row : row + head, lane] * inverse).astype(bf16)

    s = scores(0)
    for r in range(rows):
        if r + 1 < rows:
            ahead = scores(r + 1)
        attend(r, s)
        s = ahead
    second.wait()
    wot = wo[...].T

    def close(c, both):
        for k in range(2):
            r = 2 * c + k
            m = raw[r] + both[:, k * feats : (k + 1) * feats]
            mid[r] = m
            xn[r * feats : (r + 1) * feats, :] = layer_norm(m, g1).astype(bf16).T

    both = nn(wot, ctx[:, 0:step])
    for c in range(chunks):
        if c + 1 < chunks:
            ahead = nn(wot, ctx[:, (c + 1) * step : (c + 2) * step])
        close(c, both)
        both = ahead
    shape = (192, rows * 16)
    o, t = iota(shape, 0), iota(shape, 1)
    f, r = t & 15, t >> 4
    base = f * 12
    low = onehot(o == base + r)
    first_half = onehot((o == base + 8 + (r & 3)) & (r < 4))
    second_half = onehot((o == base + 8 + (r & 3)) & (r >= 4))
    lane = iota((192, 128), 1)
    for b in range(feats // 16):
        x = jnp.concatenate([xn[k * feats + b * 16 : k * feats + b * 16 + 16, :] for k in range(rows)], axis=0)
        tail = x[:, 128:width]
        tails = jnp.concatenate([tail, tail], axis=1)
        out = nn(low, x[:, 0:128]) + jnp.where(lane < 64, nn(first_half, tails), nn(second_half, tails))
        send[b * 192 : (b + 1) * 192, :] = out.astype(bf16)


def prep_kernel(after, qkv, wout, w_in, gain, wt, wo, wi, g2):
    del after
    prepare_weights(qkv, wt)
    wo[...] = wout[...].T
    wi[...] = w_in[...].T
    g2[...] = jnp.broadcast_to(column(gain[2:3, :]), g2.shape)


def rows_kernel(n_train, got, wt, send, xn, qs, ks, vs, ctx, sbuf):
    width = wt.shape[-1]
    head = width // HEADS
    total = xn.shape[0]
    fill_constant_rows(qs, vs, head)
    t, p = iota((128, 192), 0), iota((128, 192), 1)
    low = onehot(p == (t >> 3) * 12 + (t & 7))
    high = onehot(p == (t >> 3) * 12 + 8 + (t & 3))
    early = (iota((128, 64), 0) & 7) < 4
    for b in range(total // 128):
        a = got[b * 192 : (b + 1) * 192, :]
        hi = nn(high, a)
        xn[b * 128 : (b + 1) * 128, 0:128] = nn(low, a).astype(bf16)
        xn[b * 128 : (b + 1) * 128, 128:width] = jnp.where(early, hi[:, 0:64], hi[:, 64:128]).astype(bf16)
    live = n_train[0]
    step = 256
    for c in range(total // step):
        at = slice(c * step, (c + 1) * step)
        bias = jnp.where(iota((1, step), 1) + c * step < live, 0.0, masked_score)
        project(nt(wt[...], xn[at, :]), bias, at, qs, ks, vs, head)

    tiles = total // 256
    blocks = total // 256

    def score(h, cols, b):
        s = nn(ks[b * 256 : (b + 1) * 256, h * 128 : (h + 1) * 128], qs[h, :, cols])
        sbuf[h % 2, b * 256 : (b + 1) * 256, :] = s
        return jnp.max(s.reshape(32, 8, 256), axis=0)

    def columns(j):
        return pl.ds(pl.multiple_of(j * 256, 256), 256)

    peak = score(0, slice(0, 256), 0)
    for b in range(1, blocks):
        peak = jnp.maximum(peak, score(0, slice(0, 256), b))

    def query_tile(j, peak):
        cols = columns(j)
        after = columns(jnp.minimum(j + 1, tiles - 1))
        for h in range(HEADS):
            top = jnp.max(peak, axis=0, keepdims=True)
            o = None
            peak = None
            for b in range(blocks):
                ahead = score(h + 1, cols, b) if h + 1 < HEADS else score(0, after, b)
                peak = ahead if peak is None else jnp.maximum(peak, ahead)
                w = jnp.exp2(sbuf[h % 2, b * 256 : (b + 1) * 256, :] - top).astype(bf16)
                part = nn(vs[h, :, b * 256 : (b + 1) * 256], w)
                o = part if o is None else o + part
            ctx[h * head : (h + 1) * head, cols] = (o[0:head] * (1.0 / o[head : head + 1])).astype(bf16)
        return peak

    lax.fori_loop(0, tiles, query_tile, peak)
    o, q = iota((192, 128), 0), iota((192, 128), 1)
    base, r = (q >> 3) * 12, q & 7
    low = onehot(o == base + r)
    first = onehot((o == base + 8 + (r & 3)) & (r < 4))
    second = onehot((o == base + 8 + (r & 3)) & (r >= 4))
    lane = iota((192, 128), 1)
    for b in range(total // 128):
        at = slice(b * 128, (b + 1) * 128)
        tail = ctx[128:width, at]
        tails = jnp.concatenate([tail, tail], axis=0)
        out = nt(low, ctx[0:128, at]) + jnp.where(lane < 64, nt(first, tails), nt(second, tails))
        send[b * 192 : (b + 1) * 192, :] = out.astype(bf16)


def tail_kernel(got, mid, g2, wo, wi, w_out, result, ctx, out_buf, sems):
    rows, width, feats = mid.shape
    t, p = iota((128, 192), 0), iota((128, 192), 1)
    low = onehot(p == (t & 15) * 12 + (t >> 4))
    high = onehot(p == (t & 15) * 12 + 8 + ((t >> 4) & 3))
    early = iota((128, 64), 0) < 64
    for b in range(feats // 16):
        a = got[b * 192 : (b + 1) * 192, :]
        hi = nn(high, a)
        lo = nn(low, a).astype(bf16)
        hi = jnp.where(early, hi[:, 0:64], hi[:, 64:128]).astype(bf16)
        for r in range(rows):
            at = slice(r * feats + b * 16, r * feats + b * 16 + 16)
            ctx[at, 0:128] = lo[r * 16 : (r + 1) * 16]
            ctx[at, 128:width] = hi[r * 16 : (r + 1) * 16]
    sent = []
    for c in range(rows // 2):
        old = jnp.concatenate([mid[2 * c], mid[2 * c + 1]], axis=1)
        late = old + nt(wo[...], ctx[c * 2 * feats : (c + 1) * 2 * feats, :])
        n3 = layer_norm(late, g2[...]).astype(bf16)
        z = nn(wi[...], n3)
        hidden = (z * 0.5 * (1.0 + lax.erf(z * math.sqrt(0.5)))).astype(bf16)
        out = late + nn(w_out[...], hidden)
        for k in range(2):
            out_buf[2 * c + k] = out[:, k * feats : (k + 1) * feats]
            sent.append(pltpu.make_async_copy(out_buf.at[2 * c + k], result.at[2 * c + k], sems.at[2 * c + k]))
            sent[-1].start()
    for s in sent:
        s.wait()


VMEM = pl.BlockSpec(memory_space=pltpu.VMEM)
SMEM = pl.BlockSpec(memory_space=pltpu.SMEM)
ANY = pl.BlockSpec(memory_space=pl.ANY)


def near(x):
    return pltpu.with_memory_space_constraint(x, pltpu.VMEM)


def front(present, cells, gain, qkv, wout):
    rows, width, feats = cells.shape
    head = width // HEADS
    tokens = rows * feats
    return pl.pallas_call(
        front_kernel,
        out_shape=(
            pltpu.VMEM(cells.shape, f32),
            pltpu.VMEM((tokens * width // 128, 128), bf16),
        ),
        in_specs=[VMEM, ANY, VMEM, ANY, ANY],
        out_specs=(VMEM, VMEM),
        scratch_shapes=[
            pltpu.VMEM(cells.shape, f32),
            pltpu.VMEM(qkv.shape, bf16),
            pltpu.VMEM(wout.shape, bf16),
            pltpu.VMEM((tokens, width), bf16),
            pltpu.VMEM((HEADS // 2, 8 * head, 2 * tokens), bf16),
            pltpu.VMEM((tokens, HEADS * 128), bf16),
            pltpu.VMEM((HEADS * (head + 16), tokens), bf16),
            pltpu.VMEM((width, tokens), bf16),
            pltpu.VMEM((3 * width, width), bf16),
            pltpu.SemaphoreType.DMA((rows,)),
            pltpu.SemaphoreType.DMA((2,)),
        ],
        name="front",
    )(present, cells, gain, qkv, wout)


def prep(after, qkv, wout, w_in, gain):
    width, hidden = w_in.shape
    return pl.pallas_call(
        prep_kernel,
        out_shape=(
            pltpu.VMEM((3 * width, width), bf16),
            pltpu.VMEM((width, width), bf16),
            pltpu.VMEM((hidden, width), bf16),
            pltpu.VMEM((width, 256), f32),
        ),
        in_specs=[VMEM] * 5,
        out_specs=(VMEM, VMEM, VMEM, VMEM),
        name="prep",
    )(near(after), qkv, wout, w_in, gain)


def rows(n_train, got, wt):
    width = wt.shape[-1]
    head = width // HEADS
    tokens = got.shape[0] * 128 // width
    return pl.pallas_call(
        rows_kernel,
        out_shape=pltpu.VMEM(got.shape, bf16),
        in_specs=[SMEM, VMEM, VMEM],
        out_specs=VMEM,
        scratch_shapes=[
            pltpu.VMEM((tokens, width), bf16),
            pltpu.VMEM((HEADS, 4 * head, tokens), bf16),
            pltpu.VMEM((tokens, HEADS * 128), bf16),
            pltpu.VMEM((HEADS, head + 16, tokens), bf16),
            pltpu.VMEM((width, tokens), bf16),
            pltpu.VMEM((2, tokens, 256), f32),
        ],
        name="rows",
    )(n_train, near(got), near(wt))


def tail(got, mid, g2, wo, wi, w_out):
    rows, width, feats = mid.shape
    return pl.pallas_call(
        tail_kernel,
        out_shape=jax.ShapeDtypeStruct(mid.shape, f32),
        in_specs=[VMEM] * 6,
        out_specs=ANY,
        scratch_shapes=[
            pltpu.VMEM((rows * feats, width), bf16),
            pltpu.VMEM(mid.shape, f32),
            pltpu.SemaphoreType.DMA((rows,)),
        ],
        name="tail",
    )(near(got), near(mid), near(g2), near(wo), near(wi), near(w_out))


def exchanged(block):
    peers = lax.axis_size(ROW)
    tiles = block.reshape(peers, 3, 4, 128)
    return lax.all_to_all(tiles, ROW, 0, 0, tiled=True).reshape(block.shape)


def body(
    cells, n_train, present, norm_gain, feat_qkv, feat_out, item_qkv, item_out, mlp_in, mlp_out
):
    stood = jnp.transpose(cells, (0, 2, 1))
    mid, send = front(present.reshape(1, -1), stood, norm_gain, feat_qkv, feat_out)
    wt, wo, wi, g2 = prep(mid, item_qkv, item_out, mlp_in, norm_gain)
    got = exchanged(send)
    back = rows(n_train, got, wt)
    returned = exchanged(back)
    out = tail(returned, mid, g2, wo, wi, jnp.transpose(mlp_out))
    return jnp.transpose(out, (0, 2, 1))


def solution(mesh):
    return jax.shard_map(
        body,
        mesh=mesh,
        in_specs=(P(GRP_ROW, None, None), P("grp"), P("grp"), P(), P(), P(), P(), P(), P(), P()),
        out_specs=P(GRP_ROW, None, None),
        check_vma=False,
    )
```

```python
import math

import jax
import jax.numpy as jnp
from jax import lax
from jax.experimental import pallas as pl
from jax.experimental.pallas import tpu as pltpu
from jax.sharding import PartitionSpec as P

HEADS = 6
ROW = "row"
GRP_ROW = ("grp", "row")
f32 = jnp.float32
bf16 = jnp.bfloat16

norm_floor = 0.25
masked_score = -1e30


def nn(a, b):
    return lax.dot_general(a, b, (((1,), (0,)), ((), ())), preferred_element_type=f32)


def nt(a, b):
    return lax.dot_general(a, b, (((1,), (1,)), ((), ())), preferred_element_type=f32)


def tn(a, b):
    return lax.dot_general(a, b, (((0,), (0,)), ((), ())), preferred_element_type=f32)


def iota(shape, dim):
    return lax.broadcasted_iota(jnp.int32, shape, dim)


def onehot(mask):
    return jnp.where(mask, 1.0, 0.0).astype(bf16)


def layer_norm(v, gain):
    scale = 1.0 / v.shape[0]
    mean = jnp.sum(v, axis=0, keepdims=True) * scale
    c = v - mean
    var = jnp.sum(c * c, axis=0, keepdims=True) * scale
    return c * lax.rsqrt(var + norm_floor) * gain


def column(row):
    n = row.shape[-1]
    eye = iota((n, n), 0) == iota((n, n), 1)
    return jnp.sum(jnp.where(eye, row, 0.0), axis=1, keepdims=True)


def prepare_weights(qkv, wt):
    width = qkv.shape[-1]
    for c in range(3):
        wt[c * width : (c + 1) * width, :] = qkv[c].T


def fill_constant_rows(qs, vs, head):
    cols = qs.shape[-1]
    one_row = onehot(iota((head, cols), 0) == 0)
    for h in range(HEADS):
        qs[h, 3 * head : 4 * head, :] = one_row
        vs[h, head : head + 16, :] = jnp.ones((16, cols), bf16)


def split(v):
    hi = v.astype(bf16)
    return hi, (v - hi.astype(f32)).astype(bf16)


def project(triple, bias, rows, qs, ks, vs, head):
    width = triple.shape[0] // 3
    scale = (1.0 / math.sqrt(head)) * math.log2(math.e)
    qh, ql = split(triple[0:width] * scale)
    kh, kl = split(triple[width : 2 * width])
    v = triple[2 * width : 3 * width].astype(bf16)
    shape = (head, triple.shape[1])
    last = jnp.where(iota(shape, 0) == 0, bias, 0.0).astype(bf16)
    for h in range(HEADS):
        mine = slice(h * head, (h + 1) * head)
        qs[h, 0:head, rows] = qh[mine]
        qs[h, head : 2 * head, rows] = ql[mine]
        qs[h, 2 * head : 3 * head, rows] = qh[mine]
        vs[h, 0:head, rows] = v[mine]
        stack = jnp.concatenate([kh[mine], kh[mine], kl[mine], last], axis=0)
        ks[rows, h * 128 : (h + 1) * 128] = stack.T


def front_kernel(
    present, cells, gain, qkv, wout, mid, send, raw, wq, wo, live, gains, packed, xn, qs, ks, vs, ctx, wt, cell_sems, sems, out_sems
):
    rows, width, feats = cells.shape
    head = width // HEADS
    step = 2 * feats
    chunks = rows // 2
    copies = [pltpu.make_async_copy(cells.at[r], raw.at[r], cell_sems.at[r]) for r in range(rows)]
    first = pltpu.make_async_copy(qkv, wq, sems.at[0])
    second = pltpu.make_async_copy(wout, wo, sems.at[1])
    third = pltpu.make_async_copy(gain, gains, sems.at[2])
    fourth = pltpu.make_async_copy(present, live, sems.at[3])
    third.start()
    fourth.start()
    first.start()
    copies[0].start()
    copies[1].start()
    for c in copies[2:]:
        c.start()
    second.start()
    for p in range(HEADS // 2):
        for r in range(rows):
            qs[p, 0:128, r * step + feats : (r + 1) * step] = jnp.zeros((128, feats), bf16)
            qs[p, 128:256, r * step : r * step + feats] = jnp.zeros((128, feats), bf16)
            one_row = onehot(iota((head, feats), 0) == 0)
            qs[p, 3 * head : 4 * head, r * step : r * step + feats] = one_row
            qs[p, 7 * head : 8 * head, r * step + feats : (r + 1) * step] = one_row
    for h in range(HEADS):
        at = h * (head + 16) + head
        vs[at : at + 16, :] = jnp.ones((16, rows * feats), bf16)
    for c in (third, fourth, first, *copies, second):
        c.wait()
    g0 = jnp.broadcast_to(column(gains[0:1, :]), (width, feats))
    g1 = jnp.broadcast_to(column(gains[1:2, :]), (width, feats))
    bias = jnp.where(live[...] > 0, 0.0, masked_score)
    bias = jnp.concatenate([bias, bias], axis=1)
    last = jnp.where(iota((head, step), 0) == 0, bias, 0.0).astype(bf16)
    prepare_weights(wq, wt)
    wot = wo[...].T
    scale = (1.0 / math.sqrt(head)) * math.log2(math.e)

    def normed(c):
        return jnp.concatenate([layer_norm(raw[2 * c + k], g0).astype(bf16) for k in range(2)], axis=1)

    def place(c, triple):
        tok = slice(c * step, (c + 1) * step)
        qh, ql = split(triple[0:width] * scale)
        kh, kl = split(triple[width : 2 * width])
        v = triple[2 * width : 3 * width].astype(bf16)
        for h in range(HEADS):
            mine = slice(h * head, (h + 1) * head)
            vs[h * (head + 16) : h * (head + 16) + head, tok] = v[mine]
            up = (h % 2) * 128
            for k in range(2):
                col = (2 * c + k) * step + (h % 2) * feats
                part = slice(k * feats, (k + 1) * feats)
                qs[h // 2, up : up + head, col : col + feats] = qh[mine, part]
                qs[h // 2, up + head : up + 2 * head, col : col + feats] = ql[mine, part]
                qs[h // 2, up + 2 * head : up + 3 * head, col : col + feats] = qh[mine, part]
            ks[tok, h * 128 : (h + 1) * 128] = jnp.concatenate([kh[mine], kh[mine], kl[mine], last], axis=0).T

    def scores(r):
        at = slice(r * feats, (r + 1) * feats)
        return [nn(ks[at, p * 256 : (p + 1) * 256], qs[p, :, r * step : (r + 1) * step]) for p in range(HEADS // 2)]

    def attend(r, s):
        at = slice(r * feats, (r + 1) * feats)
        w = [jnp.exp2(x - jnp.max(x, axis=0, keepdims=True)).astype(bf16) for x in s]
        for p in range(HEADS // 2):
            o = nn(vs[p * 2 * (head + 16) : (p + 1) * 2 * (head + 16), at], w[p])
            for k in range(2):
                lane, row = slice(k * feats, (k + 1) * feats), k * (head + 16)
                h = 2 * p + k
                inverse = 1.0 / o[row + head : row + head + 1, lane]
                ctx[h * head : (h + 1) * head, at] = (o[row : row + head, lane] * inverse).astype(bf16)

    def close(c, both):
        for k in range(2):
            r = 2 * c + k
            m = raw[r] + both[:, k * feats : (k + 1) * feats]
            mid[r] = m
            xn[r * feats : (r + 1) * feats, :] = layer_norm(m, g1).astype(bf16).T

    triples, found, both = {}, {}, {}
    for t in range(chunks + 3):
        if t < chunks:
            triples[t] = nn(wt[...], normed(t))
        if 0 <= t - 2 < chunks:
            for r in (2 * t - 4, 2 * t - 3):
                attend(r, found.pop(r))
            both[t - 2] = nn(wot, ctx[:, (t - 2) * step : (t - 1) * step])
        if 0 <= t - 1 < chunks:
            place(t - 1, triples.pop(t - 1))
            for r in (2 * t - 2, 2 * t - 1):
                found[r] = scores(r)
        if 0 <= t - 3 < chunks:
            close(t - 3, both.pop(t - 3))
    shape = (192, rows * 16)
    o, t = iota(shape, 0), iota(shape, 1)
    f, r = t & 15, t >> 4
    base = f * 12
    low = onehot(o == base + r)
    first_half = onehot((o == base + 8 + (r & 3)) & (r < 4))
    second_half = onehot((o == base + 8 + (r & 3)) & (r >= 4))
    lane = iota((192, 128), 1)
    sent = []
    for b in range(feats // 16):
        x = jnp.concatenate([xn[k * feats + b * 16 : k * feats + b * 16 + 16, :] for k in range(rows)], axis=0)
        tail = x[:, 128:width]
        tails = jnp.concatenate([tail, tail], axis=1)
        out = nn(low, x[:, 0:128]) + jnp.where(lane < 64, nn(first_half, tails), nn(second_half, tails))
        at = slice(b * 192, (b + 1) * 192)
        packed[at, :] = out.astype(bf16)
        sent.append(pltpu.make_async_copy(packed.at[at, :], send.at[at, :], out_sems.at[b]))
        sent[-1].start()
    for c in sent:
        c.wait()


def prep_kernel(after, qkv, wout, w_in, gain, wt, wo, wi, g2):
    del after
    prepare_weights(qkv, wt)
    wo[...] = wout[...].T
    wi[...] = w_in[...].T
    g2[...] = jnp.broadcast_to(column(gain[2:3, :]), g2.shape)


def rows_kernel(n_train, got, wt, send, xn, qs, ks, vs, ctx, sbuf):
    width = wt.shape[-1]
    head = width // HEADS
    total = xn.shape[0]
    fill_constant_rows(qs, vs, head)
    t, p = iota((128, 192), 0), iota((128, 192), 1)
    low = onehot(p == (t >> 3) * 12 + (t & 7))
    high = onehot(p == (t >> 3) * 12 + 8 + (t & 3))
    early = (iota((128, 64), 0) & 7) < 4
    for b in range(total // 128):
        a = got[b * 192 : (b + 1) * 192, :]
        hi = nn(high, a)
        xn[b * 128 : (b + 1) * 128, 0:128] = nn(low, a).astype(bf16)
        xn[b * 128 : (b + 1) * 128, 128:width] = jnp.where(early, hi[:, 0:64], hi[:, 64:128]).astype(bf16)
    live = n_train[0]
    step = 256
    for c in range(total // step):
        at = slice(c * step, (c + 1) * step)
        bias = jnp.where(iota((1, step), 1) + c * step < live, 0.0, masked_score)
        project(nt(wt[...], xn[at, :]), bias, at, qs, ks, vs, head)

    tiles = total // 256
    blocks = total // 512

    def score(h, cols, b):
        s = nn(ks[b * 512 : (b + 1) * 512, h * 128 : (h + 1) * 128], qs[h, :, cols])
        sbuf[h % 2, b * 512 : (b + 1) * 512, :] = s
        return jnp.max(s.reshape(512 // 8, 8, 256), axis=0)

    def columns(j):
        return pl.ds(pl.multiple_of(j * 256, 256), 256)

    def gather(h, b, w, o):
        part = nn(vs[h, :, b * 512 : (b + 1) * 512], w)
        return part if o is None else o + part

    def finish(h, cols, o):
        ctx[h * head : (h + 1) * head, cols] = (o[0:head] * (1.0 / o[head : head + 1])).astype(bf16)

    peak = score(0, slice(0, 256), 0)
    for b in range(1, blocks):
        peak = jnp.maximum(peak, score(0, slice(0, 256), b))

    def query_tile(j, peak):
        cols = columns(j)
        after = columns(jnp.minimum(j + 1, tiles - 1))
        held = []
        o = None
        for h in range(HEADS):
            top = jnp.max(peak, axis=0, keepdims=True)
            peak = None
            for b in range(blocks):
                ahead = score(h + 1, cols, b) if h + 1 < HEADS else score(0, after, b)
                peak = ahead if peak is None else jnp.maximum(peak, ahead)
                held.append((h, b, jnp.exp2(sbuf[h % 2, b * 512 : (b + 1) * 512, :] - top).astype(bf16)))
                while len(held) > 1:
                    hh, bb, w = held.pop(0)
                    o = gather(hh, bb, w, None if bb == 0 else o)
                    if bb == blocks - 1:
                        finish(hh, cols, o)
        for hh, bb, w in held:
            o = gather(hh, bb, w, None if bb == 0 else o)
            if bb == blocks - 1:
                finish(hh, cols, o)
        return peak

    lax.fori_loop(0, tiles, query_tile, peak)
    o, q = iota((192, 128), 0), iota((192, 128), 1)
    base, r = (q >> 3) * 12, q & 7
    low = onehot(o == base + r)
    first = onehot((o == base + 8 + (r & 3)) & (r < 4))
    second = onehot((o == base + 8 + (r & 3)) & (r >= 4))
    lane = iota((192, 128), 1)
    for b in range(total // 128):
        at = slice(b * 128, (b + 1) * 128)
        tail = ctx[128:width, at]
        tails = jnp.concatenate([tail, tail], axis=0)
        out = nt(low, ctx[0:128, at]) + jnp.where(lane < 64, nt(first, tails), nt(second, tails))
        send[b * 192 : (b + 1) * 192, :] = out.astype(bf16)


def tail_kernel(got, mid, g2, wo, wi, w_out, result, ctx, out_buf, sems):
    rows, width, feats = mid.shape
    t, p = iota((128, 192), 0), iota((128, 192), 1)
    low = onehot(p == (t & 15) * 12 + (t >> 4))
    high = onehot(p == (t & 15) * 12 + 8 + ((t >> 4) & 3))
    early = iota((128, 64), 0) < 64
    for b in range(feats // 16):
        a = got[b * 192 : (b + 1) * 192, :]
        hi = nn(high, a)
        lo = nn(low, a).astype(bf16)
        hi = jnp.where(early, hi[:, 0:64], hi[:, 64:128]).astype(bf16)
        for r in range(rows):
            at = slice(r * feats + b * 16, r * feats + b * 16 + 16)
            ctx[at, 0:128] = lo[r * 16 : (r + 1) * 16]
            ctx[at, 128:width] = hi[r * 16 : (r + 1) * 16]
    sent = []
    chunks = rows // 2
    late, z, hidden = {}, {}, {}
    for t in range(chunks + 3):
        if t < chunks:
            old = jnp.concatenate([mid[2 * t], mid[2 * t + 1]], axis=1)
            late[t] = old + nt(wo[...], ctx[t * 2 * feats : (t + 1) * 2 * feats, :])
        if 0 <= t - 2 < chunks:
            v = z.pop(t - 2)
            hidden[t - 2] = (v * 0.5 * (1.0 + lax.erf(v * math.sqrt(0.5)))).astype(bf16)
        if 0 <= t - 1 < chunks:
            z[t - 1] = nn(wi[...], layer_norm(late[t - 1], g2[...]).astype(bf16))
        if 0 <= t - 3 < chunks:
            c = t - 3
            out = late.pop(c) + nn(w_out[...], hidden.pop(c))
            for k in range(2):
                out_buf[2 * c + k] = out[:, k * feats : (k + 1) * feats]
                sent.append(pltpu.make_async_copy(out_buf.at[2 * c + k], result.at[2 * c + k], sems.at[2 * c + k]))
                sent[-1].start()
    for s in sent:
        s.wait()


VMEM = pl.BlockSpec(memory_space=pltpu.VMEM)
SMEM = pl.BlockSpec(memory_space=pltpu.SMEM)
ANY = pl.BlockSpec(memory_space=pl.ANY)


def near(x):
    return pltpu.with_memory_space_constraint(x, pltpu.VMEM)


def front(present, cells, gain, qkv, wout):
    rows, width, feats = cells.shape
    head = width // HEADS
    tokens = rows * feats
    return pl.pallas_call(
        front_kernel,
        out_shape=(
            pltpu.VMEM(cells.shape, f32),
            jax.ShapeDtypeStruct((tokens * width // 128, 128), bf16),
        ),
        in_specs=[ANY] * 5,
        out_specs=(VMEM, ANY),
        scratch_shapes=[
            pltpu.VMEM(cells.shape, f32),
            pltpu.VMEM(qkv.shape, bf16),
            pltpu.VMEM(wout.shape, bf16),
            pltpu.VMEM(present.shape, jnp.int32),
            pltpu.VMEM(gain.shape, f32),
            pltpu.VMEM((tokens * width // 128, 128), bf16),
            pltpu.VMEM((tokens, width), bf16),
            pltpu.VMEM((HEADS // 2, 8 * head, 2 * tokens), bf16),
            pltpu.VMEM((tokens, HEADS * 128), bf16),
            pltpu.VMEM((HEADS * (head + 16), tokens), bf16),
            pltpu.VMEM((width, tokens), bf16),
            pltpu.VMEM((3 * width, width), bf16),
            pltpu.SemaphoreType.DMA((rows,)),
            pltpu.SemaphoreType.DMA((4,)),
            pltpu.SemaphoreType.DMA((feats // 16,)),
        ],
        name="front",
    )(present, cells, gain, qkv, wout)


def prep(after, qkv, wout, w_in, gain):
    width, hidden = w_in.shape
    return pl.pallas_call(
        prep_kernel,
        out_shape=(
            pltpu.VMEM((3 * width, width), bf16),
            pltpu.VMEM((width, width), bf16),
            pltpu.VMEM((hidden, width), bf16),
            pltpu.VMEM((width, 256), f32),
        ),
        in_specs=[VMEM] * 5,
        out_specs=(VMEM, VMEM, VMEM, VMEM),
        name="prep",
    )(near(after), qkv, wout, w_in, gain)


def rows(n_train, got, wt):
    width = wt.shape[-1]
    head = width // HEADS
    tokens = got.shape[0] * 128 // width
    return pl.pallas_call(
        rows_kernel,
        out_shape=pltpu.VMEM(got.shape, bf16),
        in_specs=[SMEM, VMEM, VMEM],
        out_specs=VMEM,
        scratch_shapes=[
            pltpu.VMEM((tokens, width), bf16),
            pltpu.VMEM((HEADS, 4 * head, tokens), bf16),
            pltpu.VMEM((tokens, HEADS * 128), bf16),
            pltpu.VMEM((HEADS, head + 16, tokens), bf16),
            pltpu.VMEM((width, tokens), bf16),
            pltpu.VMEM((2, tokens, 256), f32),
        ],
        name="rows",
    )(n_train, near(got), near(wt))


def tail(got, mid, g2, wo, wi, w_out):
    rows, width, feats = mid.shape
    return pl.pallas_call(
        tail_kernel,
        out_shape=jax.ShapeDtypeStruct(mid.shape, f32),
        in_specs=[VMEM] * 6,
        out_specs=ANY,
        scratch_shapes=[
            pltpu.VMEM((rows * feats, width), bf16),
            pltpu.VMEM(mid.shape, f32),
            pltpu.SemaphoreType.DMA((rows,)),
        ],
        name="tail",
    )(near(got), near(mid), near(g2), near(wo), near(wi), near(w_out))


def exchanged(block):
    peers = lax.axis_size(ROW)
    tiles = block.reshape(peers, 3, 4, 128)
    return lax.all_to_all(tiles, ROW, 0, 0, tiled=True).reshape(block.shape)


def body(
    cells, n_train, present, norm_gain, feat_qkv, feat_out, item_qkv, item_out, mlp_in, mlp_out
):
    stood = jnp.transpose(cells, (0, 2, 1))
    mid, send = front(present.reshape(1, -1), stood, norm_gain, feat_qkv, feat_out)
    wt, wo, wi, g2 = prep(mid, item_qkv, item_out, mlp_in, norm_gain)
    got = exchanged(send)
    back = rows(n_train, got, wt)
    returned = exchanged(back)
    out = tail(returned, mid, g2, wo, wi, jnp.transpose(mlp_out))
    return jnp.transpose(out, (0, 2, 1))


def solution(mesh):
    return jax.shard_map(
        body,
        mesh=mesh,
        in_specs=(P(GRP_ROW, None, None), P("grp"), P("grp"), P(), P(), P(), P(), P(), P(), P()),
        out_specs=P(GRP_ROW, None, None),
        check_vma=False,
    )
```

```python
import math

import jax
import jax.numpy as jnp
from jax import lax
from jax.experimental import pallas as pl
from jax.experimental.pallas import tpu as pltpu
from jax.sharding import PartitionSpec as P

HEADS = 6
ROW = "row"
GRP_ROW = ("grp", "row")
f32 = jnp.float32
bf16 = jnp.bfloat16

norm_floor = 0.25
masked_score = -1e30


def nn(a, b):
    return lax.dot_general(a, b, (((1,), (0,)), ((), ())), preferred_element_type=f32)


def nt(a, b):
    return lax.dot_general(a, b, (((1,), (1,)), ((), ())), preferred_element_type=f32)


def tn(a, b):
    return lax.dot_general(a, b, (((0,), (0,)), ((), ())), preferred_element_type=f32)


def iota(shape, dim):
    return lax.broadcasted_iota(jnp.int32, shape, dim)


def onehot(mask):
    return jnp.where(mask, 1.0, 0.0).astype(bf16)


def layer_norm(v, gain):
    scale = 1.0 / v.shape[0]
    mean = jnp.sum(v, axis=0, keepdims=True) * scale
    c = v - mean
    var = jnp.sum(c * c, axis=0, keepdims=True) * scale
    return c * lax.rsqrt(var + norm_floor) * gain


def column(row):
    n = row.shape[-1]
    eye = iota((n, n), 0) == iota((n, n), 1)
    return jnp.sum(jnp.where(eye, row, 0.0), axis=1, keepdims=True)


def prepare_weights(qkv, wt):
    width = qkv.shape[-1]
    for c in range(3):
        wt[c * width : (c + 1) * width, :] = qkv[c].T


def fill_constant_rows(qs, vs, head):
    cols = qs.shape[-1]
    one_row = onehot(iota((head, cols), 0) == 0)
    for h in range(HEADS):
        qs[h, 3 * head : 4 * head, :] = one_row
        vs[h, head : head + 16, :] = jnp.ones((16, cols), bf16)


def split(v):
    hi = v.astype(bf16)
    return hi, (v - hi.astype(f32)).astype(bf16)


def project(triple, bias, rows, qs, ks, vs, head):
    width = triple.shape[0] // 3
    scale = (1.0 / math.sqrt(head)) * math.log2(math.e)
    qh, ql = split(triple[0:width] * scale)
    kh, kl = split(triple[width : 2 * width])
    v = triple[2 * width : 3 * width].astype(bf16)
    shape = (head, triple.shape[1])
    last = jnp.where(iota(shape, 0) == 0, bias, 0.0).astype(bf16)
    for h in range(HEADS):
        mine = slice(h * head, (h + 1) * head)
        qs[h, 0:head, rows] = qh[mine]
        qs[h, head : 2 * head, rows] = ql[mine]
        qs[h, 2 * head : 3 * head, rows] = qh[mine]
        vs[h, 0:head, rows] = v[mine]
        stack = jnp.concatenate([kh[mine], kh[mine], kl[mine], last], axis=0)
        ks[rows, h * 128 : (h + 1) * 128] = stack.T


def swapped(v):
    return pltpu.roll(v, 4, axis=1)


def opened(block):
    a = block.astype(f32).reshape(-1, 24, 128)
    upper = iota((a.shape[0], 8, 128), 1) < 4
    v0, v1, v2 = a[:, 0:8], a[:, 8:16], a[:, 16:24]
    v3 = swapped(jnp.where(upper, v2, v1))
    h = jnp.where(upper, v1, v2)
    turned = pltpu.roll(h, 64, axis=2)
    d0 = jnp.where(upper, h, swapped(turned))
    d1 = jnp.where(upper, swapped(h), turned)
    low = jnp.concatenate([v0, v3], axis=1).reshape(-1, 128)
    high = jnp.concatenate([d0, d1], axis=1).reshape(-1, 128)
    return low.astype(bf16), high[:, 0:64].astype(bf16)


def closed(low, twice):
    low = low.reshape(-1, 16, 128)
    twice = twice.reshape(-1, 16, 128)
    shape = (low.shape[0], 8, 128)
    upper, left = iota(shape, 1) < 4, iota(shape, 2) < 64
    d0, d1 = twice[:, 0:8], twice[:, 8:16]
    h = jnp.where(upper, jnp.where(left, d0, swapped(d0)), jnp.where(left, swapped(d1), d1))
    v3 = swapped(low[:, 8:16])
    out = jnp.concatenate([low[:, 0:8], jnp.where(upper, h, v3), jnp.where(upper, v3, h)], axis=1)
    return out.reshape(-1, 128).astype(bf16)


def front_kernel(
    present, cells, gain, qkv, wout, mid, send, raw, wq, wo, live, gains, packed, xn, qs, ks, vs, ctx, wt, cell_sems, sems, out_sems
):
    rows, width, feats = cells.shape
    head = width // HEADS
    step = 2 * feats
    chunks = rows // 2
    copies = [pltpu.make_async_copy(cells.at[r], raw.at[r], cell_sems.at[r]) for r in range(rows)]
    first = pltpu.make_async_copy(qkv, wq, sems.at[0])
    second = pltpu.make_async_copy(wout, wo, sems.at[1])
    third = pltpu.make_async_copy(gain, gains, sems.at[2])
    fourth = pltpu.make_async_copy(present, live, sems.at[3])
    third.start()
    fourth.start()
    first.start()
    copies[0].start()
    copies[1].start()
    for c in copies[2:]:
        c.start()
    second.start()
    for p in range(HEADS // 2):
        for r in range(rows):
            qs[p, 0:128, r * step + feats : (r + 1) * step] = jnp.zeros((128, feats), bf16)
            qs[p, 128:256, r * step : r * step + feats] = jnp.zeros((128, feats), bf16)
            one_row = onehot(iota((head, feats), 0) == 0)
            qs[p, 3 * head : 4 * head, r * step : r * step + feats] = one_row
            qs[p, 7 * head : 8 * head, r * step + feats : (r + 1) * step] = one_row
    for h in range(HEADS):
        at = h * (head + 16) + head
        vs[at : at + 16, :] = jnp.ones((16, rows * feats), bf16)
    for c in (third, fourth, first, *copies, second):
        c.wait()
    g0 = jnp.broadcast_to(column(gains[0:1, :]), (width, feats))
    g1 = jnp.broadcast_to(column(gains[1:2, :]), (width, feats))
    bias = jnp.where(live[...] > 0, 0.0, masked_score)
    bias = jnp.concatenate([bias, bias], axis=1)
    last = jnp.where(iota((head, step), 0) == 0, bias, 0.0).astype(bf16)
    prepare_weights(wq, wt)
    wot = wo[...].T
    scale = (1.0 / math.sqrt(head)) * math.log2(math.e)

    def normed(c):
        return jnp.concatenate([layer_norm(raw[2 * c + k], g0).astype(bf16) for k in range(2)], axis=1)

    def place(c, triple):
        tok = slice(c * step, (c + 1) * step)
        qh, ql = split(triple[0:width] * scale)
        kh, kl = split(triple[width : 2 * width])
        v = triple[2 * width : 3 * width].astype(bf16)
        for h in range(HEADS):
            mine = slice(h * head, (h + 1) * head)
            vs[h * (head + 16) : h * (head + 16) + head, tok] = v[mine]
            up = (h % 2) * 128
            for k in range(2):
                col = (2 * c + k) * step + (h % 2) * feats
                part = slice(k * feats, (k + 1) * feats)
                qs[h // 2, up : up + head, col : col + feats] = qh[mine, part]
                qs[h // 2, up + head : up + 2 * head, col : col + feats] = ql[mine, part]
                qs[h // 2, up + 2 * head : up + 3 * head, col : col + feats] = qh[mine, part]
            ks[tok, h * 128 : (h + 1) * 128] = jnp.concatenate([kh[mine], kh[mine], kl[mine], last], axis=0).T

    def scores(r):
        at = slice(r * feats, (r + 1) * feats)
        return [nn(ks[at, p * 256 : (p + 1) * 256], qs[p, :, r * step : (r + 1) * step]) for p in range(HEADS // 2)]

    def attend(r, s):
        at = slice(r * feats, (r + 1) * feats)
        w = [jnp.exp2(x - jnp.max(x, axis=0, keepdims=True)).astype(bf16) for x in s]
        for p in range(HEADS // 2):
            o = nn(vs[p * 2 * (head + 16) : (p + 1) * 2 * (head + 16), at], w[p])
            for k in range(2):
                lane, row = slice(k * feats, (k + 1) * feats), k * (head + 16)
                h = 2 * p + k
                inverse = 1.0 / o[row + head : row + head + 1, lane]
                ctx[h * head : (h + 1) * head, at] = (o[row : row + head, lane] * inverse).astype(bf16)

    def close(c, both):
        for k in range(2):
            r = 2 * c + k
            m = raw[r] + both[:, k * feats : (k + 1) * feats]
            mid[r] = m
            xn[r * feats : (r + 1) * feats, :] = layer_norm(m, g1).astype(bf16).T

    triples, found, both = {}, {}, {}
    for t in range(chunks + 3):
        if t < chunks:
            triples[t] = nn(wt[...], normed(t))
        if 0 <= t - 2 < chunks:
            for r in (2 * t - 4, 2 * t - 3):
                attend(r, found.pop(r))
            both[t - 2] = nn(wot, ctx[:, (t - 2) * step : (t - 1) * step])
        if 0 <= t - 1 < chunks:
            place(t - 1, triples.pop(t - 1))
            for r in (2 * t - 2, 2 * t - 1):
                found[r] = scores(r)
        if 0 <= t - 3 < chunks:
            close(t - 3, both.pop(t - 3))
    shape = (16 * rows, 16 * rows)
    to, of = iota(shape, 0), iota(shape, 1)
    order = onehot(of == (to % rows) * 16 + to // rows)
    sent = []
    for b in range(feats // 16):
        x = jnp.concatenate([xn[k * feats + b * 16 : k * feats + b * 16 + 16, :] for k in range(rows)], axis=0)
        moved = nn(order, jnp.concatenate([x, x[:, 128:width]], axis=1))
        out = closed(moved[:, 0:128], moved[:, 128:256])
        at = slice(b * 192, (b + 1) * 192)
        packed[at, :] = out
        sent.append(pltpu.make_async_copy(packed.at[at, :], send.at[at, :], out_sems.at[b]))
        sent[-1].start()
    for c in sent:
        c.wait()


def prep_kernel(after, qkv, wout, w_in, gain, wt, wo, wi, g2):
    del after
    prepare_weights(qkv, wt)
    wo[...] = wout[...].T
    wi[...] = w_in[...].T
    g2[...] = jnp.broadcast_to(column(gain[2:3, :]), g2.shape)


def rows_kernel(n_train, got, wt, send, xn, qs, ks, vs, ctx, sbuf):
    width = wt.shape[-1]
    head = width // HEADS
    total = xn.shape[0]
    fill_constant_rows(qs, vs, head)
    live = n_train[0]
    step = 256

    def arrived(c):
        for b in (2 * c, 2 * c + 1):
            lo, hi = opened(got[b * 192 : (b + 1) * 192, :])
            xn[b * 128 : (b + 1) * 128, 0:128] = lo
            xn[b * 128 : (b + 1) * 128, 128:width] = hi
        return nt(wt[...], xn[c * step : (c + 1) * step, :])

    triple = arrived(0)
    for c in range(total // step):
        if c + 1 < total // step:
            ahead = arrived(c + 1)
        bias = jnp.where(iota((1, step), 1) + c * step < live, 0.0, masked_score)
        project(triple, bias, slice(c * step, (c + 1) * step), qs, ks, vs, head)
        triple = ahead
    tiles = total // 256
    blocks = total // 512

    def score(h, cols, b):
        s = nn(ks[b * 512 : (b + 1) * 512, h * 128 : (h + 1) * 128], qs[h, :, cols])
        sbuf[h % 2, b * 512 : (b + 1) * 512, :] = s
        return jnp.max(s.reshape(512 // 8, 8, 256), axis=0)

    def columns(j):
        return pl.ds(pl.multiple_of(j * 256, 256), 256)

    def gather(h, b, w, o):
        part = nn(vs[h, :, b * 512 : (b + 1) * 512], w)
        return part if o is None else o + part

    def finish(h, cols, o):
        ctx[h * head : (h + 1) * head, cols] = (o[0:head] * (1.0 / o[head : head + 1])).astype(bf16)

    peak = score(0, slice(0, 256), 0)
    for b in range(1, blocks):
        peak = jnp.maximum(peak, score(0, slice(0, 256), b))

    def query_tile(j, peak):
        cols = columns(j)
        after = columns(jnp.minimum(j + 1, tiles - 1))
        held = []
        o = None
        for h in range(HEADS):
            top = jnp.max(peak, axis=0, keepdims=True)
            peak = None
            for b in range(blocks):
                ahead = score(h + 1, cols, b) if h + 1 < HEADS else score(0, after, b)
                peak = ahead if peak is None else jnp.maximum(peak, ahead)
                held.append((h, b, jnp.exp2(sbuf[h % 2, b * 512 : (b + 1) * 512, :] - top).astype(bf16)))
                while len(held) > 1:
                    hh, bb, w = held.pop(0)
                    o = gather(hh, bb, w, None if bb == 0 else o)
                    if bb == blocks - 1:
                        finish(hh, cols, o)
        for hh, bb, w in held:
            o = gather(hh, bb, w, None if bb == 0 else o)
            if bb == blocks - 1:
                finish(hh, cols, o)
        return peak

    lax.fori_loop(0, tiles, query_tile, peak)
    for b in range(total // 128):
        at = slice(b * 128, (b + 1) * 128)
        end = ctx[128:width, at]
        twice = jnp.concatenate([end, end], axis=0).T
        send[b * 192 : (b + 1) * 192, :] = closed(ctx[0:128, at].T.astype(f32), twice.astype(f32))


def tail_kernel(got, mid, g2, wo, wi, w_out, result, ctx, out_buf, sems):
    rows, width, feats = mid.shape
    shape = (16 * rows, 16 * rows)
    to, of = iota(shape, 0), iota(shape, 1)
    order = onehot(of == (to % 16) * rows + to // 16)
    for b in range(feats // 16):
        lo, hi = opened(got[b * 192 : (b + 1) * 192, :])
        x = nn(order, jnp.concatenate([lo, hi], axis=1)).astype(bf16)
        for r in range(rows):
            at = slice(r * feats + b * 16, r * feats + b * 16 + 16)
            ctx[at, :] = x[r * 16 : (r + 1) * 16]
    sent = []
    chunks = rows // 2
    late, z, hidden = {}, {}, {}
    for t in range(chunks + 3):
        if t < chunks:
            old = jnp.concatenate([mid[2 * t], mid[2 * t + 1]], axis=1)
            late[t] = old + nt(wo[...], ctx[t * 2 * feats : (t + 1) * 2 * feats, :])
        if 0 <= t - 2 < chunks:
            v = z.pop(t - 2)
            hidden[t - 2] = (v * 0.5 * (1.0 + lax.erf(v * math.sqrt(0.5)))).astype(bf16)
        if 0 <= t - 1 < chunks:
            z[t - 1] = nn(wi[...], layer_norm(late[t - 1], g2[...]).astype(bf16))
        if 0 <= t - 3 < chunks:
            c = t - 3
            out = late.pop(c) + nn(w_out[...], hidden.pop(c))
            for k in range(2):
                out_buf[2 * c + k] = out[:, k * feats : (k + 1) * feats]
                sent.append(pltpu.make_async_copy(out_buf.at[2 * c + k], result.at[2 * c + k], sems.at[2 * c + k]))
                sent[-1].start()
    for s in sent:
        s.wait()


VMEM = pl.BlockSpec(memory_space=pltpu.VMEM)
SMEM = pl.BlockSpec(memory_space=pltpu.SMEM)
ANY = pl.BlockSpec(memory_space=pl.ANY)


def near(x):
    return pltpu.with_memory_space_constraint(x, pltpu.VMEM)


def front(present, cells, gain, qkv, wout):
    rows, width, feats = cells.shape
    head = width // HEADS
    tokens = rows * feats
    return pl.pallas_call(
        front_kernel,
        out_shape=(
            pltpu.VMEM(cells.shape, f32),
            jax.ShapeDtypeStruct((tokens * width // 128, 128), bf16),
        ),
        in_specs=[ANY] * 5,
        out_specs=(VMEM, ANY),
        scratch_shapes=[
            pltpu.VMEM(cells.shape, f32),
            pltpu.VMEM(qkv.shape, bf16),
            pltpu.VMEM(wout.shape, bf16),
            pltpu.VMEM(present.shape, jnp.int32),
            pltpu.VMEM(gain.shape, f32),
            pltpu.VMEM((tokens * width // 128, 128), bf16),
            pltpu.VMEM((tokens, width), bf16),
            pltpu.VMEM((HEADS // 2, 8 * head, 2 * tokens), bf16),
            pltpu.VMEM((tokens, HEADS * 128), bf16),
            pltpu.VMEM((HEADS * (head + 16), tokens), bf16),
            pltpu.VMEM((width, tokens), bf16),
            pltpu.VMEM((3 * width, width), bf16),
            pltpu.SemaphoreType.DMA((rows,)),
            pltpu.SemaphoreType.DMA((4,)),
            pltpu.SemaphoreType.DMA((feats // 16,)),
        ],
        name="front",
    )(present, cells, gain, qkv, wout)


def prep(after, qkv, wout, w_in, gain):
    width, hidden = w_in.shape
    return pl.pallas_call(
        prep_kernel,
        out_shape=(
            pltpu.VMEM((3 * width, width), bf16),
            pltpu.VMEM((width, width), bf16),
            pltpu.VMEM((hidden, width), bf16),
            pltpu.VMEM((width, 256), f32),
        ),
        in_specs=[VMEM] * 5,
        out_specs=(VMEM, VMEM, VMEM, VMEM),
        name="prep",
    )(near(after), qkv, wout, w_in, gain)


def rows(n_train, got, wt):
    width = wt.shape[-1]
    head = width // HEADS
    tokens = got.shape[0] * 128 // width
    return pl.pallas_call(
        rows_kernel,
        out_shape=pltpu.VMEM(got.shape, bf16),
        in_specs=[SMEM, VMEM, VMEM],
        out_specs=VMEM,
        scratch_shapes=[
            pltpu.VMEM((tokens, width), bf16),
            pltpu.VMEM((HEADS, 4 * head, tokens), bf16),
            pltpu.VMEM((tokens, HEADS * 128), bf16),
            pltpu.VMEM((HEADS, head + 16, tokens), bf16),
            pltpu.VMEM((width, tokens), bf16),
            pltpu.VMEM((2, tokens, 256), f32),
        ],
        name="rows",
    )(n_train, near(got), near(wt))


def tail(got, mid, g2, wo, wi, w_out):
    rows, width, feats = mid.shape
    return pl.pallas_call(
        tail_kernel,
        out_shape=jax.ShapeDtypeStruct(mid.shape, f32),
        in_specs=[VMEM] * 6,
        out_specs=ANY,
        scratch_shapes=[
            pltpu.VMEM((rows * feats, width), bf16),
            pltpu.VMEM(mid.shape, f32),
            pltpu.SemaphoreType.DMA((rows,)),
        ],
        name="tail",
    )(near(got), near(mid), near(g2), near(wo), near(wi), near(w_out))


def exchanged(block):
    peers = lax.axis_size(ROW)
    tiles = block.reshape(peers, 3, 4, 128)
    return lax.all_to_all(tiles, ROW, 0, 0, tiled=True).reshape(block.shape)


def body(
    cells, n_train, present, norm_gain, feat_qkv, feat_out, item_qkv, item_out, mlp_in, mlp_out
):
    stood = jnp.transpose(cells, (0, 2, 1))
    mid, send = front(present.reshape(1, -1), stood, norm_gain, feat_qkv, feat_out)
    wt, wo, wi, g2 = prep(mid, item_qkv, item_out, mlp_in, norm_gain)
    got = exchanged(send)
    back = rows(n_train, got, wt)
    returned = exchanged(back)
    out = tail(returned, mid, g2, wo, wi, jnp.transpose(mlp_out))
    return jnp.transpose(out, (0, 2, 1))


def solution(mesh):
    return jax.shard_map(
        body,
        mesh=mesh,
        in_specs=(P(GRP_ROW, None, None), P("grp"), P("grp"), P(), P(), P(), P(), P(), P(), P()),
        out_specs=P(GRP_ROW, None, None),
        check_vma=False,
    )
```

```python
import functools
import math

import jax
import jax.numpy as jnp
from jax import lax
from jax.experimental import pallas as pl
from jax.experimental.pallas import tpu as pltpu
from jax.sharding import PartitionSpec as P

HEADS = 6
ROW = "row"
GRP_ROW = ("grp", "row")
f32 = jnp.float32
bf16 = jnp.bfloat16

norm_floor = 0.25
masked_score = -1e30


def nn(a, b):
    return lax.dot_general(a, b, (((1,), (0,)), ((), ())), preferred_element_type=f32)


def nt(a, b):
    return lax.dot_general(a, b, (((1,), (1,)), ((), ())), preferred_element_type=f32)


def tn(a, b):
    return lax.dot_general(a, b, (((0,), (0,)), ((), ())), preferred_element_type=f32)


def iota(shape, dim):
    return lax.broadcasted_iota(jnp.int32, shape, dim)


def onehot(mask):
    return jnp.where(mask, 1.0, 0.0).astype(bf16)


def layer_norm(v, gain):
    scale = 1.0 / v.shape[0]
    mean = jnp.sum(v, axis=0, keepdims=True) * scale
    c = v - mean
    var = jnp.sum(c * c, axis=0, keepdims=True) * scale
    return c * lax.rsqrt(var + norm_floor) * gain


def column(row):
    n = row.shape[-1]
    eye = iota((n, n), 0) == iota((n, n), 1)
    return jnp.sum(jnp.where(eye, row, 0.0), axis=1, keepdims=True)


def prepare_weights(qkv, wt):
    width = qkv.shape[-1]
    for c in range(3):
        wt[c * width : (c + 1) * width, :] = qkv[c].T


def fill_constant_rows(qs, vs, head):
    cols = qs.shape[-1]
    one_row = onehot(iota((head, cols), 0) == 0)
    for h in range(HEADS):
        qs[h, 3 * head : 4 * head, :] = one_row
        vs[h, head : head + 16, :] = jnp.ones((16, cols), bf16)


def split(v):
    hi = v.astype(bf16)
    return hi, (v - hi.astype(f32)).astype(bf16)


def project(triple, bias, rows, qs, ks, vs, head):
    width = triple.shape[0] // 3
    scale = (1.0 / math.sqrt(head)) * math.log2(math.e)
    qh, ql = split(triple[0:width] * scale)
    kh, kl = split(triple[width : 2 * width])
    v = triple[2 * width : 3 * width].astype(bf16)
    shape = (head, triple.shape[1])
    last = jnp.where(iota(shape, 0) == 0, bias, 0.0).astype(bf16)
    for h in range(HEADS):
        mine = slice(h * head, (h + 1) * head)
        qs[h, 0:head, rows] = qh[mine]
        qs[h, head : 2 * head, rows] = ql[mine]
        qs[h, 2 * head : 3 * head, rows] = qh[mine]
        vs[h, 0:head, rows] = v[mine]
        stack = jnp.concatenate([kh[mine], kh[mine], kl[mine], last], axis=0)
        ks[rows, h * 128 : (h + 1) * 128] = stack.T


def swapped(v):
    return pltpu.roll(v, 4, axis=1)


def opened(block):
    a = block.astype(f32).reshape(-1, 24, 128)
    upper = iota((a.shape[0], 8, 128), 1) < 4
    v0, v1, v2 = a[:, 0:8], a[:, 8:16], a[:, 16:24]
    v3 = swapped(jnp.where(upper, v2, v1))
    h = jnp.where(upper, v1, v2)
    turned = pltpu.roll(h, 64, axis=2)
    d0 = jnp.where(upper, h, swapped(turned))
    d1 = jnp.where(upper, swapped(h), turned)
    low = jnp.concatenate([v0, v3], axis=1).reshape(-1, 128)
    high = jnp.concatenate([d0, d1], axis=1).reshape(-1, 128)
    return low.astype(bf16), high[:, 0:64].astype(bf16)


def closed(low, twice):
    low = low.reshape(-1, 16, 128)
    twice = twice.reshape(-1, 16, 128)
    shape = (low.shape[0], 8, 128)
    upper, left = iota(shape, 1) < 4, iota(shape, 2) < 64
    d0, d1 = twice[:, 0:8], twice[:, 8:16]
    h = jnp.where(upper, jnp.where(left, d0, swapped(d0)), jnp.where(left, swapped(d1), d1))
    v3 = swapped(low[:, 8:16])
    out = jnp.concatenate([low[:, 0:8], jnp.where(upper, h, v3), jnp.where(upper, v3, h)], axis=1)
    return out.reshape(-1, 128).astype(bf16)


def front_kernel(
    present, cells, gain, qkv, wout, mid, send, raw, wq, wo, live, gains, packed, xn, qs, ks, vs, ctx, wt, cell_sems, sems, out_sems
):
    rows, width, feats = cells.shape
    head = width // HEADS
    step = 2 * feats
    chunks = rows // 2
    copies = [pltpu.make_async_copy(cells.at[r], raw.at[r], cell_sems.at[r]) for r in range(rows)]
    first = pltpu.make_async_copy(qkv, wq, sems.at[0])
    second = pltpu.make_async_copy(wout, wo, sems.at[1])
    third = pltpu.make_async_copy(gain, gains, sems.at[2])
    fourth = pltpu.make_async_copy(present, live, sems.at[3])
    third.start()
    fourth.start()
    first.start()
    copies[0].start()
    copies[1].start()
    for c in copies[2:]:
        c.start()
    second.start()
    for p in range(HEADS // 2):
        for r in range(rows):
            qs[p, 0:128, r * step + feats : (r + 1) * step] = jnp.zeros((128, feats), bf16)
            qs[p, 128:256, r * step : r * step + feats] = jnp.zeros((128, feats), bf16)
            one_row = onehot(iota((head, feats), 0) == 0)
            qs[p, 3 * head : 4 * head, r * step : r * step + feats] = one_row
            qs[p, 7 * head : 8 * head, r * step + feats : (r + 1) * step] = one_row
    for h in range(HEADS):
        at = h * (head + 16) + head
        vs[at : at + 16, :] = jnp.ones((16, rows * feats), bf16)
    for c in (third, fourth, first, *copies, second):
        c.wait()
    g0 = jnp.broadcast_to(column(gains[0:1, :]), (width, feats))
    g1 = jnp.broadcast_to(column(gains[1:2, :]), (width, feats))
    bias = jnp.where(live[...] > 0, 0.0, masked_score)
    bias = jnp.concatenate([bias, bias], axis=1)
    last = jnp.where(iota((head, step), 0) == 0, bias, 0.0).astype(bf16)
    prepare_weights(wq, wt)
    wot = wo[...].T
    scale = (1.0 / math.sqrt(head)) * math.log2(math.e)

    def normed(c):
        return jnp.concatenate([layer_norm(raw[2 * c + k], g0).astype(bf16) for k in range(2)], axis=1)

    def place(c, triple):
        tok = slice(c * step, (c + 1) * step)
        qh, ql = split(triple[0:width] * scale)
        kh, kl = split(triple[width : 2 * width])
        v = triple[2 * width : 3 * width].astype(bf16)
        for h in range(HEADS):
            mine = slice(h * head, (h + 1) * head)
            vs[h * (head + 16) : h * (head + 16) + head, tok] = v[mine]
            up = (h % 2) * 128
            for k in range(2):
                col = (2 * c + k) * step + (h % 2) * feats
                part = slice(k * feats, (k + 1) * feats)
                qs[h // 2, up : up + head, col : col + feats] = qh[mine, part]
                qs[h // 2, up + head : up + 2 * head, col : col + feats] = ql[mine, part]
                qs[h // 2, up + 2 * head : up + 3 * head, col : col + feats] = qh[mine, part]
            ks[tok, h * 128 : (h + 1) * 128] = jnp.concatenate([kh[mine], kh[mine], kl[mine], last], axis=0).T

    def scores(r):
        at = slice(r * feats, (r + 1) * feats)
        return [nn(ks[at, p * 256 : (p + 1) * 256], qs[p, :, r * step : (r + 1) * step]) for p in range(HEADS // 2)]

    def attend(r, s):
        at = slice(r * feats, (r + 1) * feats)
        w = [jnp.exp2(x - jnp.max(x, axis=0, keepdims=True)).astype(bf16) for x in s]
        for p in range(HEADS // 2):
            o = nn(vs[p * 2 * (head + 16) : (p + 1) * 2 * (head + 16), at], w[p])
            for k in range(2):
                lane, row = slice(k * feats, (k + 1) * feats), k * (head + 16)
                h = 2 * p + k
                inverse = 1.0 / o[row + head : row + head + 1, lane]
                ctx[h * head : (h + 1) * head, at] = (o[row : row + head, lane] * inverse).astype(bf16)

    def close(c, both):
        for k in range(2):
            r = 2 * c + k
            m = raw[r] + both[:, k * feats : (k + 1) * feats]
            mid[r] = m
            xn[r * feats : (r + 1) * feats, :] = layer_norm(m, g1).astype(bf16).T

    triples, found, both = {}, {}, {}
    for t in range(chunks + 3):
        if t < chunks:
            triples[t] = nn(wt[...], normed(t))
        if 0 <= t - 2 < chunks:
            for r in (2 * t - 4, 2 * t - 3):
                attend(r, found.pop(r))
            both[t - 2] = nn(wot, ctx[:, (t - 2) * step : (t - 1) * step])
        if 0 <= t - 1 < chunks:
            place(t - 1, triples.pop(t - 1))
            for r in (2 * t - 2, 2 * t - 1):
                found[r] = scores(r)
        if 0 <= t - 3 < chunks:
            close(t - 3, both.pop(t - 3))
    shape = (16 * rows, 16 * rows)
    to, of = iota(shape, 0), iota(shape, 1)
    order = onehot(of == (to % rows) * 16 + to // rows)
    sent = []
    for b in range(feats // 16):
        x = jnp.concatenate([xn[k * feats + b * 16 : k * feats + b * 16 + 16, :] for k in range(rows)], axis=0)
        moved = nn(order, jnp.concatenate([x, x[:, 128:width]], axis=1))
        out = closed(moved[:, 0:128], moved[:, 128:256])
        at = slice(b * 192, (b + 1) * 192)
        packed[at, :] = out
        sent.append(pltpu.make_async_copy(packed.at[at, :], send.at[at, :], out_sems.at[b]))
        sent[-1].start()
    for c in sent:
        c.wait()


def prep_kernel(after, qkv, wout, w_in, gain, wt, wo, wi, g2):
    del after
    prepare_weights(qkv, wt)
    wo[...] = wout[...].T
    wi[...] = w_in[...].T
    g2[...] = jnp.broadcast_to(column(gain[2:3, :]), g2.shape)


def rows_kernel(n_train, got, wt, send, xn, qs, ks, vs, ctx, sbuf):
    width = wt.shape[-1]
    head = width // HEADS
    total = xn.shape[0]
    fill_constant_rows(qs, vs, head)
    live = n_train[0]
    step = 256

    def arrived(c):
        for b in (2 * c, 2 * c + 1):
            lo, hi = opened(got[b * 192 : (b + 1) * 192, :])
            xn[b * 128 : (b + 1) * 128, 0:128] = lo
            xn[b * 128 : (b + 1) * 128, 128:width] = hi
        return nt(wt[...], xn[c * step : (c + 1) * step, :])

    triple = arrived(0)
    for c in range(total // step):
        if c + 1 < total // step:
            ahead = arrived(c + 1)
        bias = jnp.where(iota((1, step), 1) + c * step < live, 0.0, masked_score)
        project(triple, bias, slice(c * step, (c + 1) * step), qs, ks, vs, head)
        triple = ahead
    tiles = total // 256
    deep = sbuf.shape[0]

    def columns(j):
        return pl.ds(pl.multiple_of(j * 256, 256), 256)

    def score(h, cols, b):
        s = nn(ks[b * 256 : (b + 1) * 256, h * 128 : (h + 1) * 128], qs[h, :, cols])
        sbuf[h % deep, b * 256 : (b + 1) * 256, :] = s
        return jnp.max(s.reshape(32, 8, 256), axis=0)

    def gather(h, b, w, o):
        part = nn(vs[h, :, b * 256 : (b + 1) * 256], w)
        return part if o is None else o + part

    def finish(h, cols, o):
        ctx[h * head : (h + 1) * head, cols] = (o[0:head] * (1.0 / o[head : head + 1])).astype(bf16)

    def attend(blocks):
        peaks = []
        for h in range(deep - 1):
            found = [score(h, slice(0, 256), b) for b in range(blocks)]
            peaks.append(functools.reduce(jnp.maximum, found))

        def query_tile(j, peaks):
            cols = columns(j)
            after = columns(jnp.minimum(j + 1, tiles - 1))
            held = []
            o = None
            peaks = list(peaks)

            def settle(o):
                h, b, w = held.pop(0)
                o = gather(h, b, w, None if b == 0 else o)
                if b == blocks - 1:
                    finish(h, cols, o)
                return o

            for h in range(HEADS):
                top = jnp.max(peaks.pop(0), axis=0, keepdims=True)
                n = h + deep - 1
                found = []
                for b in range(blocks):
                    found.append(score(n % HEADS, cols if n < HEADS else after, b))
                    held.append((h, b, jnp.exp2(sbuf[h % deep, b * 256 : (b + 1) * 256, :] - top).astype(bf16)))
                    if len(held) > 1:
                        o = settle(o)
                peaks.append(functools.reduce(jnp.maximum, found))
            settle(o)
            return tuple(peaks)

        lax.fori_loop(0, tiles, query_tile, tuple(peaks), unroll=2)

    for blocks in range(1, total // 256 + 1):
        pl.when((live + 255) // 256 == blocks)(functools.partial(attend, blocks))
    for b in range(total // 128):
        at = slice(b * 128, (b + 1) * 128)
        end = ctx[128:width, at]
        twice = jnp.concatenate([end, end], axis=0).T
        send[b * 192 : (b + 1) * 192, :] = closed(ctx[0:128, at].T.astype(f32), twice.astype(f32))


def tail_kernel(got, mid, g2, wo, wi, w_out, result, ctx, out_buf, sems):
    rows, width, feats = mid.shape
    shape = (16 * rows, 16 * rows)
    to, of = iota(shape, 0), iota(shape, 1)
    order = onehot(of == (to % 16) * rows + to // 16)
    for b in range(feats // 16):
        lo, hi = opened(got[b * 192 : (b + 1) * 192, :])
        x = nn(order, jnp.concatenate([lo, hi], axis=1)).astype(bf16)
        for r in range(rows):
            at = slice(r * feats + b * 16, r * feats + b * 16 + 16)
            ctx[at, :] = x[r * 16 : (r + 1) * 16]
    sent = []
    chunks = rows // 2
    late, z, hidden = {}, {}, {}
    for t in range(chunks + 3):
        if t < chunks:
            old = jnp.concatenate([mid[2 * t], mid[2 * t + 1]], axis=1)
            late[t] = old + nt(wo[...], ctx[t * 2 * feats : (t + 1) * 2 * feats, :])
        if 0 <= t - 2 < chunks:
            v = z.pop(t - 2)
            hidden[t - 2] = (v * 0.5 * (1.0 + lax.erf(v * math.sqrt(0.5)))).astype(bf16)
        if 0 <= t - 1 < chunks:
            z[t - 1] = nn(wi[...], layer_norm(late[t - 1], g2[...]).astype(bf16))
        if 0 <= t - 3 < chunks:
            c = t - 3
            out = late.pop(c) + nn(w_out[...], hidden.pop(c))
            for k in range(2):
                out_buf[2 * c + k] = out[:, k * feats : (k + 1) * feats]
                sent.append(pltpu.make_async_copy(out_buf.at[2 * c + k], result.at[2 * c + k], sems.at[2 * c + k]))
                sent[-1].start()
    for s in sent:
        s.wait()


VMEM = pl.BlockSpec(memory_space=pltpu.VMEM)
SMEM = pl.BlockSpec(memory_space=pltpu.SMEM)
ANY = pl.BlockSpec(memory_space=pl.ANY)


def near(x):
    return pltpu.with_memory_space_constraint(x, pltpu.VMEM)


def front(present, cells, gain, qkv, wout):
    rows, width, feats = cells.shape
    head = width // HEADS
    tokens = rows * feats
    return pl.pallas_call(
        front_kernel,
        out_shape=(
            pltpu.VMEM(cells.shape, f32),
            jax.ShapeDtypeStruct((tokens * width // 128, 128), bf16),
        ),
        in_specs=[ANY] * 5,
        out_specs=(VMEM, ANY),
        scratch_shapes=[
            pltpu.VMEM(cells.shape, f32),
            pltpu.VMEM(qkv.shape, bf16),
            pltpu.VMEM(wout.shape, bf16),
            pltpu.VMEM(present.shape, jnp.int32),
            pltpu.VMEM(gain.shape, f32),
            pltpu.VMEM((tokens * width // 128, 128), bf16),
            pltpu.VMEM((tokens, width), bf16),
            pltpu.VMEM((HEADS // 2, 8 * head, 2 * tokens), bf16),
            pltpu.VMEM((tokens, HEADS * 128), bf16),
            pltpu.VMEM((HEADS * (head + 16), tokens), bf16),
            pltpu.VMEM((width, tokens), bf16),
            pltpu.VMEM((3 * width, width), bf16),
            pltpu.SemaphoreType.DMA((rows,)),
            pltpu.SemaphoreType.DMA((4,)),
            pltpu.SemaphoreType.DMA((feats // 16,)),
        ],
        name="front",
    )(present, cells, gain, qkv, wout)


def prep(after, qkv, wout, w_in, gain):
    width, hidden = w_in.shape
    return pl.pallas_call(
        prep_kernel,
        out_shape=(
            pltpu.VMEM((3 * width, width), bf16),
            pltpu.VMEM((width, width), bf16),
            pltpu.VMEM((hidden, width), bf16),
            pltpu.VMEM((width, 256), f32),
        ),
        in_specs=[VMEM] * 5,
        out_specs=(VMEM, VMEM, VMEM, VMEM),
        name="prep",
    )(near(after), qkv, wout, w_in, gain)


def rows(n_train, got, wt):
    width = wt.shape[-1]
    head = width // HEADS
    tokens = got.shape[0] * 128 // width
    return pl.pallas_call(
        rows_kernel,
        out_shape=pltpu.VMEM(got.shape, bf16),
        in_specs=[SMEM, VMEM, VMEM],
        out_specs=VMEM,
        scratch_shapes=[
            pltpu.VMEM((tokens, width), bf16),
            pltpu.VMEM((HEADS, 4 * head, tokens), bf16),
            pltpu.VMEM((tokens, HEADS * 128), bf16),
            pltpu.VMEM((HEADS, head + 16, tokens), bf16),
            pltpu.VMEM((width, tokens), bf16),
            pltpu.VMEM((3, tokens, 256), f32),
        ],
        name="rows",
    )(n_train, near(got), near(wt))


def tail(got, mid, g2, wo, wi, w_out):
    rows, width, feats = mid.shape
    return pl.pallas_call(
        tail_kernel,
        out_shape=jax.ShapeDtypeStruct(mid.shape, f32),
        in_specs=[VMEM] * 6,
        out_specs=ANY,
        scratch_shapes=[
            pltpu.VMEM((rows * feats, width), bf16),
            pltpu.VMEM(mid.shape, f32),
            pltpu.SemaphoreType.DMA((rows,)),
        ],
        name="tail",
    )(near(got), near(mid), near(g2), near(wo), near(wi), near(w_out))


def exchanged(block):
    peers = lax.axis_size(ROW)
    tiles = block.reshape(peers, 3, 4, 128)
    return lax.all_to_all(tiles, ROW, 0, 0, tiled=True).reshape(block.shape)


def body(
    cells, n_train, present, norm_gain, feat_qkv, feat_out, item_qkv, item_out, mlp_in, mlp_out
):
    stood = jnp.transpose(cells, (0, 2, 1))
    mid, send = front(present.reshape(1, -1), stood, norm_gain, feat_qkv, feat_out)
    wt, wo, wi, g2 = prep(mid, item_qkv, item_out, mlp_in, norm_gain)
    got = exchanged(send)
    back = rows(n_train, got, wt)
    returned = exchanged(back)
    out = tail(returned, mid, g2, wo, wi, jnp.transpose(mlp_out))
    return jnp.transpose(out, (0, 2, 1))


def solution(mesh):
    return jax.shard_map(
        body,
        mesh=mesh,
        in_specs=(P(GRP_ROW, None, None), P("grp"), P("grp"), P(), P(), P(), P(), P(), P(), P()),
        out_specs=P(GRP_ROW, None, None),
        check_vma=False,
    )
```

```python
import functools
import math

import jax
import jax.numpy as jnp
from jax import lax
from jax.experimental import pallas as pl
from jax.experimental.pallas import tpu as pltpu
from jax.sharding import PartitionSpec as P

HEADS = 6
ROW = "row"
GRP_ROW = ("grp", "row")
f32 = jnp.float32
bf16 = jnp.bfloat16

norm_floor = 0.25
masked_score = -1e30


def nn(a, b):
    return lax.dot_general(a, b, (((1,), (0,)), ((), ())), preferred_element_type=f32)


def nt(a, b):
    return lax.dot_general(a, b, (((1,), (1,)), ((), ())), preferred_element_type=f32)


def tn(a, b):
    return lax.dot_general(a, b, (((0,), (0,)), ((), ())), preferred_element_type=f32)


def iota(shape, dim):
    return lax.broadcasted_iota(jnp.int32, shape, dim)


def onehot(mask):
    return jnp.where(mask, 1.0, 0.0).astype(bf16)


def layer_norm(v, gain):
    scale = 1.0 / v.shape[0]
    mean = jnp.sum(v, axis=0, keepdims=True) * scale
    c = v - mean
    var = jnp.sum(c * c, axis=0, keepdims=True) * scale
    return c * lax.rsqrt(var + norm_floor) * gain


def column(row):
    n = row.shape[-1]
    eye = iota((n, n), 0) == iota((n, n), 1)
    return jnp.sum(jnp.where(eye, row, 0.0), axis=1, keepdims=True)


def prepare_weights(qkv, wt):
    width = qkv.shape[-1]
    for c in range(3):
        wt[c * width : (c + 1) * width, :] = qkv[c].T


def fill_constant_rows(qs, vs, head):
    cols = qs.shape[-1]
    one_row = onehot(iota((head, cols), 0) == 0)
    for h in range(HEADS):
        qs[h, 3 * head : 4 * head, :] = one_row
        vs[h, head : head + 16, :] = jnp.ones((16, cols), bf16)


def split(v):
    hi = v.astype(bf16)
    return hi, (v - hi.astype(f32)).astype(bf16)


def project(triple, bias, rows, qs, ks, vs, head):
    width = triple.shape[0] // 3
    scale = (1.0 / math.sqrt(head)) * math.log2(math.e)
    qh, ql = split(triple[0:width] * scale)
    kh, kl = split(triple[width : 2 * width])
    v = triple[2 * width : 3 * width].astype(bf16)
    shape = (head, triple.shape[1])
    last = jnp.where(iota(shape, 0) == 0, bias, 0.0).astype(bf16)
    for h in range(HEADS):
        mine = slice(h * head, (h + 1) * head)
        qs[h, 0:head, rows] = qh[mine]
        qs[h, head : 2 * head, rows] = ql[mine]
        qs[h, 2 * head : 3 * head, rows] = qh[mine]
        vs[h, 0:head, rows] = v[mine]
        stack = jnp.concatenate([kh[mine], kh[mine], kl[mine], last], axis=0)
        ks[rows, h * 128 : (h + 1) * 128] = stack.T


def swapped(v):
    return pltpu.roll(v, 4, axis=1)


def opened(block):
    a = block.astype(f32).reshape(-1, 24, 128)
    upper = iota((a.shape[0], 8, 128), 1) < 4
    v0, v1, v2 = a[:, 0:8], a[:, 8:16], a[:, 16:24]
    v3 = swapped(jnp.where(upper, v2, v1))
    h = jnp.where(upper, v1, v2)
    turned = pltpu.roll(h, 64, axis=2)
    d0 = jnp.where(upper, h, swapped(turned))
    d1 = jnp.where(upper, swapped(h), turned)
    low = jnp.concatenate([v0, v3], axis=1).reshape(-1, 128)
    high = jnp.concatenate([d0, d1], axis=1).reshape(-1, 128)
    return low.astype(bf16), high[:, 0:64].astype(bf16)


def closed(low, twice):
    low = low.reshape(-1, 16, 128)
    twice = twice.reshape(-1, 16, 128)
    shape = (low.shape[0], 8, 128)
    upper, left = iota(shape, 1) < 4, iota(shape, 2) < 64
    d0, d1 = twice[:, 0:8], twice[:, 8:16]
    h = jnp.where(upper, jnp.where(left, d0, swapped(d0)), jnp.where(left, swapped(d1), d1))
    v3 = swapped(low[:, 8:16])
    out = jnp.concatenate([low[:, 0:8], jnp.where(upper, h, v3), jnp.where(upper, v3, h)], axis=1)
    return out.reshape(-1, 128).astype(bf16)


def front_kernel(
    present, cells, gain, qkv, wout, mid, send, raw, wq, wo, live, gains, packed, xn, qs, ks, vs, ctx, wt, cell_sems, sems, out_sems
):
    rows, width, feats = cells.shape
    head = width // HEADS
    step = 2 * feats
    chunks = rows // 2
    copies = [pltpu.make_async_copy(cells.at[r], raw.at[r], cell_sems.at[r]) for r in range(rows)]
    first = pltpu.make_async_copy(qkv, wq, sems.at[0])
    second = pltpu.make_async_copy(wout, wo, sems.at[1])
    third = pltpu.make_async_copy(gain, gains, sems.at[2])
    fourth = pltpu.make_async_copy(present, live, sems.at[3])
    third.start()
    fourth.start()
    first.start()
    copies[0].start()
    copies[1].start()
    for c in copies[2:]:
        c.start()
    second.start()
    for p in range(HEADS // 2):
        for r in range(rows):
            qs[p, 0:128, r * step + feats : (r + 1) * step] = jnp.zeros((128, feats), bf16)
            qs[p, 128:256, r * step : r * step + feats] = jnp.zeros((128, feats), bf16)
            one_row = onehot(iota((head, feats), 0) == 0)
            qs[p, 3 * head : 4 * head, r * step : r * step + feats] = one_row
            qs[p, 7 * head : 8 * head, r * step + feats : (r + 1) * step] = one_row
    for h in range(HEADS):
        at = h * (head + 16) + head
        vs[at : at + 16, :] = jnp.ones((16, rows * feats), bf16)
    for c in (third, fourth, first, *copies, second):
        c.wait()
    g0 = jnp.broadcast_to(column(gains[0:1, :]), (width, feats))
    g1 = jnp.broadcast_to(column(gains[1:2, :]), (width, feats))
    bias = jnp.where(live[...] > 0, 0.0, masked_score)
    bias = jnp.concatenate([bias, bias], axis=1)
    last = jnp.where(iota((head, step), 0) == 0, bias, 0.0).astype(bf16)
    prepare_weights(wq, wt)
    wot = wo[...].T
    scale = (1.0 / math.sqrt(head)) * math.log2(math.e)

    def normed(c):
        return jnp.concatenate([layer_norm(raw[2 * c + k], g0).astype(bf16) for k in range(2)], axis=1)

    def place(c, triple):
        tok = slice(c * step, (c + 1) * step)
        qh, ql = split(triple[0:width] * scale)
        kh, kl = split(triple[width : 2 * width])
        v = triple[2 * width : 3 * width].astype(bf16)
        for h in range(HEADS):
            mine = slice(h * head, (h + 1) * head)
            vs[h * (head + 16) : h * (head + 16) + head, tok] = v[mine]
            up = (h % 2) * 128
            for k in range(2):
                col = (2 * c + k) * step + (h % 2) * feats
                part = slice(k * feats, (k + 1) * feats)
                qs[h // 2, up : up + head, col : col + feats] = qh[mine, part]
                qs[h // 2, up + head : up + 2 * head, col : col + feats] = ql[mine, part]
                qs[h // 2, up + 2 * head : up + 3 * head, col : col + feats] = qh[mine, part]
            ks[tok, h * 128 : (h + 1) * 128] = jnp.concatenate([kh[mine], kh[mine], kl[mine], last], axis=0).T

    def scores(r):
        at = slice(r * feats, (r + 1) * feats)
        return [nn(ks[at, p * 256 : (p + 1) * 256], qs[p, :, r * step : (r + 1) * step]) for p in range(HEADS // 2)]

    def attend(r, s):
        at = slice(r * feats, (r + 1) * feats)
        w = [jnp.exp2(x - jnp.max(x, axis=0, keepdims=True)).astype(bf16) for x in s]
        for p in range(HEADS // 2):
            o = nn(vs[p * 2 * (head + 16) : (p + 1) * 2 * (head + 16), at], w[p])
            for k in range(2):
                lane, row = slice(k * feats, (k + 1) * feats), k * (head + 16)
                h = 2 * p + k
                inverse = 1.0 / o[row + head : row + head + 1, lane]
                ctx[h * head : (h + 1) * head, at] = (o[row : row + head, lane] * inverse).astype(bf16)

    def close(c, both):
        for k in range(2):
            r = 2 * c + k
            m = raw[r] + both[:, k * feats : (k + 1) * feats]
            mid[r] = m
            xn[r * feats : (r + 1) * feats, :] = layer_norm(m, g1).astype(bf16).T

    triples, found, both = {}, {}, {}
    for t in range(chunks + 3):
        if t < chunks:
            triples[t] = nn(wt[...], normed(t))
        if 0 <= t - 2 < chunks:
            for r in (2 * t - 4, 2 * t - 3):
                attend(r, found.pop(r))
            both[t - 2] = nn(wot, ctx[:, (t - 2) * step : (t - 1) * step])
        if 0 <= t - 1 < chunks:
            place(t - 1, triples.pop(t - 1))
            for r in (2 * t - 2, 2 * t - 1):
                found[r] = scores(r)
        if 0 <= t - 3 < chunks:
            close(t - 3, both.pop(t - 3))
    shape = (16 * rows, 16 * rows)
    to, of = iota(shape, 0), iota(shape, 1)
    order = onehot(of == (to % rows) * 16 + to // rows)
    sent = []
    for b in range(feats // 16):
        x = jnp.concatenate([xn[k * feats + b * 16 : k * feats + b * 16 + 16, :] for k in range(rows)], axis=0)
        moved = nn(order, jnp.concatenate([x, x[:, 128:width]], axis=1))
        out = closed(moved[:, 0:128], moved[:, 128:256])
        at = slice(b * 192, (b + 1) * 192)
        packed[at, :] = out
        sent.append(pltpu.make_async_copy(packed.at[at, :], send.at[at, :], out_sems.at[b]))
        sent[-1].start()
    for c in sent:
        c.wait()


def prep_kernel(after, qkv, wout, w_in, gain, wt, wo, wi, g2):
    del after
    prepare_weights(qkv, wt)
    wo[...] = wout[...].T
    wi[...] = w_in[...].T
    g2[...] = jnp.broadcast_to(column(gain[2:3, :]), g2.shape)


def rows_kernel(n_train, got, wt, send, xn, qs, ks, vs, ctx, sbuf):
    width = wt.shape[-1]
    head = width // HEADS
    total = xn.shape[0]
    fill_constant_rows(qs, vs, head)
    live = n_train[0]
    step = 256

    def arrived(c):
        for b in (2 * c, 2 * c + 1):
            lo, hi = opened(got[b * 192 : (b + 1) * 192, :])
            xn[b * 128 : (b + 1) * 128, 0:128] = lo
            xn[b * 128 : (b + 1) * 128, 128:width] = hi
        return nt(wt[...], xn[c * step : (c + 1) * step, :])

    tiles = total // 256
    deep = sbuf.shape[0]

    def columns(j):
        return pl.ds(pl.multiple_of(j * 256, 256), 256)

    def score(h, cols, b):
        s = nn(ks[b * 256 : (b + 1) * 256, h * 128 : (h + 1) * 128], qs[h, :, cols])
        sbuf[h % deep, b * 256 : (b + 1) * 256, :] = s
        return jnp.max(s.reshape(32, 8, 256), axis=0)

    triple = arrived(0)
    opening = [[] for _ in range(deep - 1)]
    for c in range(total // step):
        if c + 1 < total // step:
            ahead = arrived(c + 1)
        bias = jnp.where(iota((1, step), 1) + c * step < live, 0.0, masked_score)
        project(triple, bias, slice(c * step, (c + 1) * step), qs, ks, vs, head)
        if c > 0:
            for h in range(deep - 1):
                opening[h].append(score(h, slice(0, 256), c - 1))
        triple = ahead
    for h in range(deep - 1):
        opening[h].append(score(h, slice(0, 256), total // step - 1))
    opening = [functools.reduce(jnp.maximum, found) for found in opening]

    def gather(h, b, w, o):
        part = nn(vs[h, :, b * 256 : (b + 1) * 256], w)
        return part if o is None else o + part

    def finish(h, cols, o):
        ctx[h * head : (h + 1) * head, cols] = (o[0:head] * (1.0 / o[head : head + 1])).astype(bf16)

    def attend(blocks):
        def query_tile(j, peaks):
            cols = columns(j)
            after = columns(jnp.minimum(j + 1, tiles - 1))
            held = []
            o = None
            peaks = list(peaks)

            def settle(o):
                h, b, w = held.pop(0)
                o = gather(h, b, w, None if b == 0 else o)
                if b == blocks - 1:
                    finish(h, cols, o)
                return o

            for h in range(HEADS):
                top = jnp.max(peaks.pop(0), axis=0, keepdims=True)
                n = h + deep - 1
                found = []
                for b in range(blocks):
                    found.append(score(n % HEADS, cols if n < HEADS else after, b))
                    held.append((h, b, jnp.exp2(sbuf[h % deep, b * 256 : (b + 1) * 256, :] - top).astype(bf16)))
                    if len(held) > 1:
                        o = settle(o)
                peaks.append(functools.reduce(jnp.maximum, found))
            settle(o)
            return tuple(peaks)

        lax.fori_loop(0, tiles, query_tile, tuple(opening), unroll=2)

    for blocks in range(1, total // 256 + 1):
        pl.when((live + 255) // 256 == blocks)(functools.partial(attend, blocks))
    for b in range(total // 128):
        at = slice(b * 128, (b + 1) * 128)
        end = ctx[128:width, at]
        twice = jnp.concatenate([end, end], axis=0).T
        send[b * 192 : (b + 1) * 192, :] = closed(ctx[0:128, at].T.astype(f32), twice.astype(f32))


def tail_kernel(got, mid, g2, wo, wi, w_out, result, ctx, out_buf, sems):
    rows, width, feats = mid.shape
    shape = (16 * rows, 16 * rows)
    to, of = iota(shape, 0), iota(shape, 1)
    order = onehot(of == (to % 16) * rows + to // 16)
    for b in range(feats // 16):
        lo, hi = opened(got[b * 192 : (b + 1) * 192, :])
        x = nn(order, jnp.concatenate([lo, hi], axis=1)).astype(bf16)
        for r in range(rows):
            at = slice(r * feats + b * 16, r * feats + b * 16 + 16)
            ctx[at, :] = x[r * 16 : (r + 1) * 16]
    sent = []
    chunks = rows // 2
    late, z, hidden = {}, {}, {}
    for t in range(chunks + 3):
        if t < chunks:
            old = jnp.concatenate([mid[2 * t], mid[2 * t + 1]], axis=1)
            late[t] = old + nt(wo[...], ctx[t * 2 * feats : (t + 1) * 2 * feats, :])
        if 0 <= t - 2 < chunks:
            v = z.pop(t - 2)
            hidden[t - 2] = (v * 0.5 * (1.0 + lax.erf(v * math.sqrt(0.5)))).astype(bf16)
        if 0 <= t - 1 < chunks:
            z[t - 1] = nn(wi[...], layer_norm(late[t - 1], g2[...]).astype(bf16))
        if 0 <= t - 3 < chunks:
            c = t - 3
            out = late.pop(c) + nn(w_out[...], hidden.pop(c))
            for k in range(2):
                out_buf[2 * c + k] = out[:, k * feats : (k + 1) * feats]
                sent.append(pltpu.make_async_copy(out_buf.at[2 * c + k], result.at[2 * c + k], sems.at[2 * c + k]))
                sent[-1].start()
    for s in sent:
        s.wait()


VMEM = pl.BlockSpec(memory_space=pltpu.VMEM)
SMEM = pl.BlockSpec(memory_space=pltpu.SMEM)
ANY = pl.BlockSpec(memory_space=pl.ANY)


def near(x):
    return pltpu.with_memory_space_constraint(x, pltpu.VMEM)


def front(present, cells, gain, qkv, wout):
    rows, width, feats = cells.shape
    head = width // HEADS
    tokens = rows * feats
    return pl.pallas_call(
        front_kernel,
        out_shape=(
            pltpu.VMEM(cells.shape, f32),
            jax.ShapeDtypeStruct((tokens * width // 128, 128), bf16),
        ),
        in_specs=[ANY] * 5,
        out_specs=(VMEM, ANY),
        scratch_shapes=[
            pltpu.VMEM(cells.shape, f32),
            pltpu.VMEM(qkv.shape, bf16),
            pltpu.VMEM(wout.shape, bf16),
            pltpu.VMEM(present.shape, jnp.int32),
            pltpu.VMEM(gain.shape, f32),
            pltpu.VMEM((tokens * width // 128, 128), bf16),
            pltpu.VMEM((tokens, width), bf16),
            pltpu.VMEM((HEADS // 2, 8 * head, 2 * tokens), bf16),
            pltpu.VMEM((tokens, HEADS * 128), bf16),
            pltpu.VMEM((HEADS * (head + 16), tokens), bf16),
            pltpu.VMEM((width, tokens), bf16),
            pltpu.VMEM((3 * width, width), bf16),
            pltpu.SemaphoreType.DMA((rows,)),
            pltpu.SemaphoreType.DMA((4,)),
            pltpu.SemaphoreType.DMA((feats // 16,)),
        ],
        name="front",
    )(present, cells, gain, qkv, wout)


def prep(after, qkv, wout, w_in, gain):
    width, hidden = w_in.shape
    return pl.pallas_call(
        prep_kernel,
        out_shape=(
            pltpu.VMEM((3 * width, width), bf16),
            pltpu.VMEM((width, width), bf16),
            pltpu.VMEM((hidden, width), bf16),
            pltpu.VMEM((width, 256), f32),
        ),
        in_specs=[VMEM] * 5,
        out_specs=(VMEM, VMEM, VMEM, VMEM),
        name="prep",
    )(near(after), qkv, wout, w_in, gain)


def rows(n_train, got, wt):
    width = wt.shape[-1]
    head = width // HEADS
    tokens = got.shape[0] * 128 // width
    return pl.pallas_call(
        rows_kernel,
        out_shape=pltpu.VMEM(got.shape, bf16),
        in_specs=[SMEM, VMEM, VMEM],
        out_specs=VMEM,
        scratch_shapes=[
            pltpu.VMEM((tokens, width), bf16),
            pltpu.VMEM((HEADS, 4 * head, tokens), bf16),
            pltpu.VMEM((tokens, HEADS * 128), bf16),
            pltpu.VMEM((HEADS, head + 16, tokens), bf16),
            pltpu.VMEM((width, tokens), bf16),
            pltpu.VMEM((3, tokens, 256), f32),
        ],
        name="rows",
    )(n_train, near(got), near(wt))


def tail(got, mid, g2, wo, wi, w_out):
    rows, width, feats = mid.shape
    return pl.pallas_call(
        tail_kernel,
        out_shape=jax.ShapeDtypeStruct(mid.shape, f32),
        in_specs=[VMEM] * 6,
        out_specs=ANY,
        scratch_shapes=[
            pltpu.VMEM((rows * feats, width), bf16),
            pltpu.VMEM(mid.shape, f32),
            pltpu.SemaphoreType.DMA((rows,)),
        ],
        name="tail",
    )(near(got), near(mid), near(g2), near(wo), near(wi), near(w_out))


def exchanged(block):
    peers = lax.axis_size(ROW)
    tiles = block.reshape(peers, 3, 4, 128)
    return lax.all_to_all(tiles, ROW, 0, 0, tiled=True).reshape(block.shape)


def body(
    cells, n_train, present, norm_gain, feat_qkv, feat_out, item_qkv, item_out, mlp_in, mlp_out
):
    stood = jnp.transpose(cells, (0, 2, 1))
    mid, send = front(present.reshape(1, -1), stood, norm_gain, feat_qkv, feat_out)
    wt, wo, wi, g2 = prep(mid, item_qkv, item_out, mlp_in, norm_gain)
    got = exchanged(send)
    back = rows(n_train, got, wt)
    returned = exchanged(back)
    out = tail(returned, mid, g2, wo, wi, jnp.transpose(mlp_out))
    return jnp.transpose(out, (0, 2, 1))


def solution(mesh):
    return jax.shard_map(
        body,
        mesh=mesh,
        in_specs=(P(GRP_ROW, None, None), P("grp"), P("grp"), P(), P(), P(), P(), P(), P(), P()),
        out_specs=P(GRP_ROW, None, None),
        check_vma=False,
    )
```

```python
import functools
import math

import jax
import jax.numpy as jnp
from jax import lax
from jax.experimental import pallas as pl
from jax.experimental.pallas import tpu as pltpu
from jax.sharding import PartitionSpec as P

HEADS = 6
ROW = "row"
GRP_ROW = ("grp", "row")
f32 = jnp.float32
bf16 = jnp.bfloat16

norm_floor = 0.25
masked_score = -1e30


def nn(a, b):
    return lax.dot_general(a, b, (((1,), (0,)), ((), ())), preferred_element_type=f32)


def nt(a, b):
    return lax.dot_general(a, b, (((1,), (1,)), ((), ())), preferred_element_type=f32)


def tn(a, b):
    return lax.dot_general(a, b, (((0,), (0,)), ((), ())), preferred_element_type=f32)


def iota(shape, dim):
    return lax.broadcasted_iota(jnp.int32, shape, dim)


def onehot(mask):
    return jnp.where(mask, 1.0, 0.0).astype(bf16)


def layer_norm(v, gain):
    scale = 1.0 / v.shape[0]
    mean = jnp.sum(v, axis=0, keepdims=True) * scale
    c = v - mean
    var = jnp.sum(c * c, axis=0, keepdims=True) * scale
    return c * lax.rsqrt(var + norm_floor) * gain


def column(row):
    n = row.shape[-1]
    eye = iota((n, n), 0) == iota((n, n), 1)
    return jnp.sum(jnp.where(eye, row, 0.0), axis=1, keepdims=True)


def prepare_weights(qkv, wt):
    width = qkv.shape[-1]
    for c in range(3):
        wt[c * width : (c + 1) * width, :] = qkv[c].T


def fill_constant_rows(qs, vs, head):
    cols = qs.shape[-1]
    one_row = onehot(iota((head, cols), 0) == 0)
    for h in range(HEADS):
        qs[h, 3 * head : 4 * head, :] = one_row
        vs[h, head : head + 16, :] = jnp.ones((16, cols), bf16)


def split(v):
    hi = v.astype(bf16)
    return hi, (v - hi.astype(f32)).astype(bf16)


def project(triple, bias, rows, qs, ks, vs, head):
    width = triple.shape[0] // 3
    scale = (1.0 / math.sqrt(head)) * math.log2(math.e)
    qh, ql = split(triple[0:width] * scale)
    kh, kl = split(triple[width : 2 * width])
    v = triple[2 * width : 3 * width].astype(bf16)
    shape = (head, triple.shape[1])
    last = jnp.where(iota(shape, 0) == 0, bias, 0.0).astype(bf16)
    for h in range(HEADS):
        mine = slice(h * head, (h + 1) * head)
        qs[h, 0:head, rows] = qh[mine]
        qs[h, head : 2 * head, rows] = ql[mine]
        qs[h, 2 * head : 3 * head, rows] = qh[mine]
        vs[h, 0:head, rows] = v[mine]
        stack = jnp.concatenate([kh[mine], kh[mine], kl[mine], last], axis=0)
        ks[rows, h * 128 : (h + 1) * 128] = stack.T


def swapped(v):
    return pltpu.roll(v, 4, axis=1)


def opened(block):
    a = block.astype(f32).reshape(-1, 24, 128)
    upper = iota((a.shape[0], 8, 128), 1) < 4
    v0, v1, v2 = a[:, 0:8], a[:, 8:16], a[:, 16:24]
    v3 = swapped(jnp.where(upper, v2, v1))
    h = jnp.where(upper, v1, v2)
    turned = pltpu.roll(h, 64, axis=2)
    d0 = jnp.where(upper, h, swapped(turned))
    d1 = jnp.where(upper, swapped(h), turned)
    low = jnp.concatenate([v0, v3], axis=1).reshape(-1, 128)
    high = jnp.concatenate([d0, d1], axis=1).reshape(-1, 128)
    return low.astype(bf16), high[:, 0:64].astype(bf16)


def closed(low, twice):
    low = low.reshape(-1, 16, 128)
    twice = twice.reshape(-1, 16, 128)
    shape = (low.shape[0], 8, 128)
    upper, left = iota(shape, 1) < 4, iota(shape, 2) < 64
    d0, d1 = twice[:, 0:8], twice[:, 8:16]
    h = jnp.where(upper, jnp.where(left, d0, swapped(d0)), jnp.where(left, swapped(d1), d1))
    v3 = swapped(low[:, 8:16])
    out = jnp.concatenate([low[:, 0:8], jnp.where(upper, h, v3), jnp.where(upper, v3, h)], axis=1)
    return out.reshape(-1, 128).astype(bf16)


def front_kernel(
    present, cells, gain, qkv, wout, n_train, mid, send, g2, count, raw, wq, wo, live, gains, xn, qs, ks, vs, ctx, wt, number, cell_sems, sems
):
    rows, width, feats = cells.shape
    head = width // HEADS
    step = 2 * feats
    chunks = rows // 2
    copies = [pltpu.make_async_copy(cells.at[r], raw.at[r], cell_sems.at[r]) for r in range(rows)]
    first = pltpu.make_async_copy(qkv, wq, sems.at[0])
    second = pltpu.make_async_copy(wout, wo, sems.at[1])
    third = pltpu.make_async_copy(gain, gains, sems.at[2])
    fourth = pltpu.make_async_copy(present, live, sems.at[3])
    fifth = pltpu.make_async_copy(n_train, number, sems.at[4])
    third.start()
    fourth.start()
    fifth.start()
    first.start()
    copies[0].start()
    copies[1].start()
    for c in copies[2:]:
        c.start()
    second.start()
    for p in range(HEADS // 2):
        for r in range(rows):
            qs[p, 0:128, r * step + feats : (r + 1) * step] = jnp.zeros((128, feats), bf16)
            qs[p, 128:256, r * step : r * step + feats] = jnp.zeros((128, feats), bf16)
            one_row = onehot(iota((head, feats), 0) == 0)
            qs[p, 3 * head : 4 * head, r * step : r * step + feats] = one_row
            qs[p, 7 * head : 8 * head, r * step + feats : (r + 1) * step] = one_row
    for h in range(HEADS):
        at = h * (head + 16) + head
        vs[at : at + 16, :] = jnp.ones((16, rows * feats), bf16)
    for c in (third, fourth, fifth, first, *copies, second):
        c.wait()
    g0 = jnp.broadcast_to(column(gains[0:1, :]), (width, feats))
    g1 = jnp.broadcast_to(column(gains[1:2, :]), (width, feats))
    count[...] = jnp.full(count.shape, number[0].astype(f32), f32)
    g2[...] = jnp.broadcast_to(column(gains[2:3, :]), g2.shape)
    bias = jnp.where(live[...] > 0, 0.0, masked_score)
    bias = jnp.concatenate([bias, bias], axis=1)
    last = jnp.where(iota((head, step), 0) == 0, bias, 0.0).astype(bf16)
    prepare_weights(wq, wt)
    wot = wo[...].T
    scale = (1.0 / math.sqrt(head)) * math.log2(math.e)

    def normed(c):
        return jnp.concatenate([layer_norm(raw[2 * c + k], g0).astype(bf16) for k in range(2)], axis=1)

    def place(c, triple):
        tok = slice(c * step, (c + 1) * step)
        qh, ql = split(triple[0:width] * scale)
        kh, kl = split(triple[width : 2 * width])
        v = triple[2 * width : 3 * width].astype(bf16)
        for h in range(HEADS):
            mine = slice(h * head, (h + 1) * head)
            vs[h * (head + 16) : h * (head + 16) + head, tok] = v[mine]
            up = (h % 2) * 128
            for k in range(2):
                col = (2 * c + k) * step + (h % 2) * feats
                part = slice(k * feats, (k + 1) * feats)
                qs[h // 2, up : up + head, col : col + feats] = qh[mine, part]
                qs[h // 2, up + head : up + 2 * head, col : col + feats] = ql[mine, part]
                qs[h // 2, up + 2 * head : up + 3 * head, col : col + feats] = qh[mine, part]
            ks[tok, h * 128 : (h + 1) * 128] = jnp.concatenate([kh[mine], kh[mine], kl[mine], last], axis=0).T

    def scores(r):
        at = slice(r * feats, (r + 1) * feats)
        return [nn(ks[at, p * 256 : (p + 1) * 256], qs[p, :, r * step : (r + 1) * step]) for p in range(HEADS // 2)]

    def attend(r, s):
        at = slice(r * feats, (r + 1) * feats)
        w = [jnp.exp2(x - jnp.max(x, axis=0, keepdims=True)).astype(bf16) for x in s]
        for p in range(HEADS // 2):
            o = nn(vs[p * 2 * (head + 16) : (p + 1) * 2 * (head + 16), at], w[p])
            for k in range(2):
                lane, row = slice(k * feats, (k + 1) * feats), k * (head + 16)
                h = 2 * p + k
                inverse = 1.0 / o[row + head : row + head + 1, lane]
                ctx[h * head : (h + 1) * head, at] = (o[row : row + head, lane] * inverse).astype(bf16)

    def close(c, both):
        for k in range(2):
            r = 2 * c + k
            m = raw[r] + both[:, k * feats : (k + 1) * feats]
            mid[r] = m
            xn[r * feats : (r + 1) * feats, :] = layer_norm(m, g1).astype(bf16).T

    triples, found, both = {}, {}, {}
    for t in range(chunks + 3):
        if t < chunks:
            triples[t] = nn(wt[...], normed(t))
        if 0 <= t - 2 < chunks:
            for r in (2 * t - 4, 2 * t - 3):
                attend(r, found.pop(r))
            both[t - 2] = nn(wot, ctx[:, (t - 2) * step : (t - 1) * step])
        if 0 <= t - 1 < chunks:
            place(t - 1, triples.pop(t - 1))
            for r in (2 * t - 2, 2 * t - 1):
                found[r] = scores(r)
        if 0 <= t - 3 < chunks:
            close(t - 3, both.pop(t - 3))
    shape = (16 * rows, 16 * rows)
    to, of = iota(shape, 0), iota(shape, 1)
    order = onehot(of == (to % rows) * 16 + to // rows)
    for b in range(feats // 16):
        x = jnp.concatenate([xn[k * feats + b * 16 : k * feats + b * 16 + 16, :] for k in range(rows)], axis=0)
        moved = nn(order, jnp.concatenate([x, x[:, 128:width]], axis=1))
        out = closed(moved[:, 0:128], moved[:, 128:256])
        at = slice(b * 192, (b + 1) * 192)
        send[at, :] = out


def rows_kernel(n_train, got, qkv, send, xn, qs, ks, vs, ctx, wt, sbuf):
    width = qkv.shape[-1]
    head = width // HEADS
    total = xn.shape[0]
    prepare_weights(qkv, wt)
    fill_constant_rows(qs, vs, head)
    live = jnp.max(n_train[...]).astype(jnp.int32)
    step = 256

    def arrived(c):
        for b in (2 * c, 2 * c + 1):
            lo, hi = opened(got[b * 192 : (b + 1) * 192, :])
            xn[b * 128 : (b + 1) * 128, 0:128] = lo
            xn[b * 128 : (b + 1) * 128, 128:width] = hi
        return nt(wt[...], xn[c * step : (c + 1) * step, :])

    tiles = total // 256
    deep = sbuf.shape[0]

    def columns(j):
        return pl.ds(pl.multiple_of(j * 256, 256), 256)

    def score(h, cols, b):
        s = nn(ks[b * 256 : (b + 1) * 256, h * 128 : (h + 1) * 128], qs[h, :, cols])
        sbuf[h % deep, b * 256 : (b + 1) * 256, :] = s
        return jnp.max(s.reshape(32, 8, 256), axis=0)

    triple = arrived(0)
    opening = [[] for _ in range(deep - 1)]
    for c in range(total // step):
        if c + 1 < total // step:
            ahead = arrived(c + 1)
        bias = jnp.where(iota((1, step), 1) + c * step < live, 0.0, masked_score)
        project(triple, bias, slice(c * step, (c + 1) * step), qs, ks, vs, head)
        if c > 0:
            for h in range(deep - 1):
                opening[h].append(score(h, slice(0, 256), c - 1))
        triple = ahead
    for h in range(deep - 1):
        opening[h].append(score(h, slice(0, 256), total // step - 1))
    opening = [functools.reduce(jnp.maximum, found) for found in opening]

    def gather(h, b, w, o):
        part = nn(vs[h, :, b * 256 : (b + 1) * 256], w)
        return part if o is None else o + part

    def finish(h, cols, o):
        ctx[h * head : (h + 1) * head, cols] = (o[0:head] * (1.0 / o[head : head + 1])).astype(bf16)

    def attend(blocks):
        def query_tile(j, peaks):
            cols = columns(j)
            after = columns(jnp.minimum(j + 1, tiles - 1))
            held = []
            o = None
            peaks = list(peaks)

            def settle(o):
                h, b, w = held.pop(0)
                o = gather(h, b, w, None if b == 0 else o)
                if b == blocks - 1:
                    finish(h, cols, o)
                return o

            for h in range(HEADS):
                top = jnp.max(peaks.pop(0), axis=0, keepdims=True)
                n = h + deep - 1
                found = []
                for b in range(blocks):
                    found.append(score(n % HEADS, cols if n < HEADS else after, b))
                    held.append((h, b, jnp.exp2(sbuf[h % deep, b * 256 : (b + 1) * 256, :] - top).astype(bf16)))
                    if len(held) > 1:
                        o = settle(o)
                peaks.append(functools.reduce(jnp.maximum, found))
            settle(o)
            return tuple(peaks)

        lax.fori_loop(0, tiles, query_tile, tuple(opening), unroll=2)

    for blocks in range(1, total // 256 + 1):
        pl.when((live + 255) // 256 == blocks)(functools.partial(attend, blocks))
    for b in range(total // 128):
        at = slice(b * 128, (b + 1) * 128)
        end = ctx[128:width, at]
        twice = jnp.concatenate([end, end], axis=0).T
        send[b * 192 : (b + 1) * 192, :] = closed(ctx[0:128, at].T.astype(f32), twice.astype(f32))


def tail_kernel(got, mid, g2, wout, w_in, w_out, result, ctx, out_buf, sems):
    rows, width, feats = mid.shape
    wo = wout[...].T
    wi = w_in[...].T
    shape = (16 * rows, 16 * rows)
    to, of = iota(shape, 0), iota(shape, 1)
    order = onehot(of == (to % 16) * rows + to // 16)
    for b in range(feats // 16):
        lo, hi = opened(got[b * 192 : (b + 1) * 192, :])
        x = nn(order, jnp.concatenate([lo, hi], axis=1)).astype(bf16)
        for r in range(rows):
            at = slice(r * feats + b * 16, r * feats + b * 16 + 16)
            ctx[at, :] = x[r * 16 : (r + 1) * 16]
    sent = []
    chunks = rows // 2
    late, z, hidden = {}, {}, {}
    for t in range(chunks + 3):
        if t < chunks:
            old = jnp.concatenate([mid[2 * t], mid[2 * t + 1]], axis=1)
            late[t] = old + nt(wo, ctx[t * 2 * feats : (t + 1) * 2 * feats, :])
        if 0 <= t - 2 < chunks:
            v = z.pop(t - 2)
            hidden[t - 2] = (v * 0.5 * (1.0 + lax.erf(v * math.sqrt(0.5)))).astype(bf16)
        if 0 <= t - 1 < chunks:
            z[t - 1] = nn(wi, layer_norm(late[t - 1], g2[...]).astype(bf16))
        if 0 <= t - 3 < chunks:
            c = t - 3
            out = late.pop(c) + nn(w_out[...], hidden.pop(c))
            for k in range(2):
                out_buf[2 * c + k] = out[:, k * feats : (k + 1) * feats]
                sent.append(pltpu.make_async_copy(out_buf.at[2 * c + k], result.at[2 * c + k], sems.at[2 * c + k]))
                sent[-1].start()
    for s in sent:
        s.wait()


VMEM = pl.BlockSpec(memory_space=pltpu.VMEM)
ANY = pl.BlockSpec(memory_space=pl.ANY)


def near(x):
    return pltpu.with_memory_space_constraint(x, pltpu.VMEM)


def front(present, cells, gain, qkv, wout, n_train):
    rows, width, feats = cells.shape
    head = width // HEADS
    tokens = rows * feats
    return pl.pallas_call(
        front_kernel,
        out_shape=(
            pltpu.VMEM(cells.shape, f32),
            pltpu.VMEM((tokens * width // 128, 128), bf16),
            pltpu.VMEM((width, 2 * feats), f32),
            pltpu.VMEM((8, 128), f32),
        ),
        in_specs=[ANY] * 6,
        out_specs=(VMEM, VMEM, VMEM, VMEM),
        scratch_shapes=[
            pltpu.VMEM(cells.shape, f32),
            pltpu.VMEM(qkv.shape, bf16),
            pltpu.VMEM(wout.shape, bf16),
            pltpu.VMEM(present.shape, jnp.int32),
            pltpu.VMEM(gain.shape, f32),
            pltpu.VMEM((tokens, width), bf16),
            pltpu.VMEM((HEADS // 2, 8 * head, 2 * tokens), bf16),
            pltpu.VMEM((tokens, HEADS * 128), bf16),
            pltpu.VMEM((HEADS * (head + 16), tokens), bf16),
            pltpu.VMEM((width, tokens), bf16),
            pltpu.VMEM((3 * width, width), bf16),
            pltpu.SMEM((1,), jnp.int32),
            pltpu.SemaphoreType.DMA((rows,)),
            pltpu.SemaphoreType.DMA((5,)),
        ],
        name="front",
    )(present, cells, gain, qkv, wout, n_train)


def rows(n_train, got, qkv):
    width = qkv.shape[-1]
    head = width // HEADS
    tokens = got.shape[0] * 128 // width
    return pl.pallas_call(
        rows_kernel,
        out_shape=pltpu.VMEM(got.shape, bf16),
        in_specs=[VMEM, VMEM, VMEM],
        out_specs=VMEM,
        scratch_shapes=[
            pltpu.VMEM((tokens, width), bf16),
            pltpu.VMEM((HEADS, 4 * head, tokens), bf16),
            pltpu.VMEM((tokens, HEADS * 128), bf16),
            pltpu.VMEM((HEADS, head + 16, tokens), bf16),
            pltpu.VMEM((width, tokens), bf16),
            pltpu.VMEM((3 * width, width), bf16),
            pltpu.VMEM((3, tokens, 256), f32),
        ],
        name="rows",
    )(near(n_train), near(got), near(qkv))


def tail(got, mid, g2, wout, w_in, w_out):
    rows, width, feats = mid.shape
    return pl.pallas_call(
        tail_kernel,
        out_shape=jax.ShapeDtypeStruct(mid.shape, f32),
        in_specs=[VMEM] * 6,
        out_specs=ANY,
        scratch_shapes=[
            pltpu.VMEM((rows * feats, width), bf16),
            pltpu.VMEM(mid.shape, f32),
            pltpu.SemaphoreType.DMA((rows,)),
        ],
        name="tail",
    )(near(got), near(mid), near(g2), near(wout), near(w_in), near(w_out))


def exchanged(block):
    peers = lax.axis_size(ROW)
    tiles = block.reshape(peers, 3, 4, 128)
    return lax.all_to_all(tiles, ROW, 0, 0, tiled=True).reshape(block.shape)


def body(
    cells, n_train, present, norm_gain, feat_qkv, feat_out, item_qkv, item_out, mlp_in, mlp_out
):
    stood = jnp.transpose(cells, (0, 2, 1))
    mid, send, g2, count = front(present.reshape(1, -1), stood, norm_gain, feat_qkv, feat_out, n_train)
    got = exchanged(send)
    back = rows(count, got, item_qkv)
    returned = exchanged(back)
    out = tail(returned, mid, g2, item_out, mlp_in, jnp.transpose(mlp_out))
    return jnp.transpose(out, (0, 2, 1))


def solution(mesh):
    return jax.shard_map(
        body,
        mesh=mesh,
        in_specs=(P(GRP_ROW, None, None), P("grp"), P("grp"), P(), P(), P(), P(), P(), P(), P()),
        out_specs=P(GRP_ROW, None, None),
        check_vma=False,
    )
```
